32 devices in a mesh: dp: 8 (over z, x), var: 4 (over y, core).
Axes of the slice: x: 2, y: 2, z: 4, core: 2. Of those that a mesh axis runs over, the one named last changes fastest.
Arguments:
- pixels: bfloat16 [8, 24, 4, 256], P('dp', 'var'), may hold values from -6 to 6
- var_ids: int32 [8, 24], P('dp', 'var'), may hold values from 0 to 90, as said below
- counts: int32 [8], P('dp'), may hold values from 3 to 24, as said below
- patch_weight: bfloat16 [91, 4, 1024], replicated, may hold values from -3 to 3
- var_embed: bfloat16 [91, 1024], replicated, may hold values from -5 to 5
- norm_gain: float32 [1024], replicated, may hold values from 0.1 to 1.9
- norm_bias: float32 [1024], replicated, may hold values from -3 to 3
- key_weight: bfloat16 [1024, 1024], P('dp'), may hold values from -0.1875 to 0.1875
- value_weight: bfloat16 [1024, 1024], P('dp'), may hold values from -0.1875 to 0.1875
- query: float32 [16, 64], replicated, may hold values from -200 to 200
- out_weight: bfloat16 [1024, 1024], replicated, may hold values from -0.1875 to 0.1875
Outputs:
- aggregated: bfloat16 [8, 256, 1024], P('dp', 'var')
The draws below stay inside these ranges and needn't reach their ends.
Inputs may be any that keep to these rules, and one draw needn't show every extreme that they name: `var_ids`: in each sample the ids of slots below its count are distinct; slots at or past the count are padding with arbitrary ids. `counts`: some sample has exactly min(91, 24) live slots and some has exactly 3.
All inputs are finite; a program needn't handle non-finite values.
Results may differ from the reference program's by a relative error of at most 0.018.
Values may be sent and summed in bfloat16 or wider, within the bound.
A program may use at most 64 MiB of HBM per device.

```python
import math
import jax
import jax.numpy as jnp
from jax import lax

D = 1024
HEADS = 16
HEAD = 64
PP = 4
VARS = 91
PW = 256
BATCH = 8
VSLOTS = 24


def draw_var_ids(key, part):
    sample_keys = jax.random.split(key, BATCH)

    def one(sample_key):
        order = jax.random.permutation(sample_key, VARS).astype(jnp.int32)
        filler = jax.random.randint(jax.random.fold_in(sample_key, 7), (VSLOTS,), 0, VARS).astype(jnp.int32)
        return jnp.concatenate([order, filler])[:VSLOTS]
    return jax.vmap(one)(sample_keys)


def draw_counts(key, part):
    highest = min(VARS, VSLOTS)
    base = jax.random.randint(jax.random.fold_in(key, 11), (BATCH,), 3, highest + 1).astype(jnp.int32)
    picked = jax.random.permutation(jax.random.fold_in(key, 13), BATCH)
    base = jnp.where(picked == 0, jnp.int32(highest), base)
    base = jnp.where(picked == 1, jnp.int32(3), base)
    return base.astype(jnp.int32)


def draw_query(key, part):
    first = jax.random.fold_in(key, 21)
    second = jax.random.fold_in(key, 23)
    base = jnp.clip(jax.random.normal(first, (HEADS, HEAD), jnp.float32), -5.0, 5.0)
    scales = jnp.exp(jax.random.uniform(second, (HEADS, 1), jnp.float32, math.log(0.5), math.log(4.0)))
    return (base * scales).astype(jnp.float32)


def block_levels(rng, extent, pieces, least, top_value):
    gain, own = 1.0, jax.random.fold_in(rng, 6)
    for position, blocks in pieces:
        heights = jnp.exp(jax.random.uniform(jax.random.fold_in(own, position), (blocks,), jnp.float32, least / len(pieces), top_value / len(pieces)))
        gain = gain * jnp.repeat(heights, extent[position] // blocks).reshape([-1 if axis == position else 1 for axis in range(len(extent))])
    return gain


def bell_draw(rng, dims, width, reach, cuts=(), kind=jnp.bfloat16):
    factor_of = block_levels(rng, dims, cuts, -0.22, 0.18) if cuts else 1.0
    values = jax.random.normal(rng, dims, jnp.float32) * width * factor_of
    return jnp.minimum(jnp.maximum(values, -reach), reach).astype(kind)


def setup_inputs(seed: int = 0) -> dict:
    splits = jax.random.split(jax.random.key(seed), 12)
    pixels = bell_draw(splits[0], (BATCH, VSLOTS, PP, PW), 1.0, 6.0, ((0, 8), (1, 4)))
    var_ids = draw_var_ids(jax.random.fold_in(splits[11], 71), 0)
    counts = draw_counts(jax.random.fold_in(splits[11], 71), 0)
    patch_weight = bell_draw(splits[3], (VARS, PP, D), PP ** -0.5, 3.0)
    var_embed = bell_draw(splits[4], (VARS, D), 1.0, 5.0)
    norm_gain = jnp.clip(1.0 + 0.18 * jax.random.normal(splits[5], (D,), jnp.float32), 0.1, 1.9)
    norm_bias = bell_draw(splits[6], (D,), 0.5, 3.0, (), jnp.float32)
    key_weight = bell_draw(splits[7], (D, D), D ** -0.5, 0.1875, ((0, 8),))
    value_weight = bell_draw(splits[8], (D, D), D ** -0.5, 0.1875, ((0, 8),))
    query = draw_query(jax.random.fold_in(splits[11], 71), 0)
    out_weight = bell_draw(splits[10], (D, D), D ** -0.5, 0.1875)
    return {"pixels": pixels, "var_ids": var_ids, "counts": counts, "patch_weight": patch_weight, "var_embed": var_embed, "norm_gain": norm_gain, "norm_bias": norm_bias, "key_weight": key_weight, "value_weight": value_weight, "query": query, "out_weight": out_weight}


def one_sample(pixels, ids, count, patch_weight, var_embed, norm_gain, norm_bias, key_weight, value_weight, query, out_weight):
    table = patch_weight[ids]
    embedded = jnp.einsum('skp,skd->spd', pixels.astype(jnp.float32), table.astype(jnp.float32))
    embedded = embedded + var_embed[ids].astype(jnp.float32)[:, None, :]
    center = embedded - lax.optimization_barrier(jnp.mean(embedded, axis=-1, keepdims=True))
    spread = lax.optimization_barrier(jnp.mean(center * center, axis=-1, keepdims=True))
    normed = (center * lax.rsqrt(spread + 1e-05) * norm_gain + norm_bias).astype(jnp.bfloat16)
    slots = normed.shape[0]
    patches = normed.shape[1]
    flat = normed.reshape(slots * patches, D)
    keys = jnp.dot(flat, key_weight, preferred_element_type=jnp.float32).reshape(slots * patches, HEADS, HEAD)
    scores = jnp.einsum('nhe,he->nh', keys, query, precision=lax.Precision.HIGHEST) * (1.0 / math.sqrt(HEAD))
    scores = scores.reshape(slots, patches, HEADS)
    live = (jnp.arange(slots, dtype=jnp.int32) < count)[:, None, None]
    scores = jnp.where(live, scores, jnp.float32(-1e+30))
    peak = lax.optimization_barrier(jnp.max(scores, axis=0))
    expo = jnp.exp(scores - peak)
    total = lax.optimization_barrier(jnp.sum(expo, axis=0))
    probs = expo.astype(jnp.bfloat16)
    values = jnp.dot(flat, value_weight, preferred_element_type=jnp.float32).astype(jnp.bfloat16)
    values = values.reshape(slots, patches, HEADS, HEAD)
    numer = jnp.einsum('sph,sphe->phe', probs.astype(jnp.float32), values.astype(jnp.float32))
    mixed = (numer / total[:, :, None]).reshape(patches, D).astype(jnp.bfloat16)
    return jnp.dot(mixed, out_weight, preferred_element_type=jnp.float32).astype(jnp.bfloat16)

def reference(pixels, var_ids, counts, patch_weight, var_embed, norm_gain, norm_bias, key_weight, value_weight, query, out_weight):

    def apply(item):
        return one_sample(item[0], item[1], item[2], patch_weight, var_embed, norm_gain, norm_bias, key_weight, value_weight, query, out_weight)
    return lax.map(apply, (pixels, var_ids, counts))
```

```python
import functools
import math

import jax
import jax.numpy as jnp
from jax import lax
from jax.experimental import pallas as pl
from jax.experimental.pallas import tpu as pltpu
from jax.sharding import PartitionSpec as P

F32 = jnp.float32
BF16 = jnp.bfloat16
EXACT = lax.Precision.HIGHEST


def rounded_up(value, unit):
    return -(-value // unit) * unit


def kernel(
    dims,
    ids_hbm,
    counts_hbm,
    pixels_hbm,
    table_hbm,
    embed_hbm,
    gain_hbm,
    bias_hbm,
    key_hbm,
    value_hbm,
    query_hbm,
    out_hbm,
    result_ref,
    ids_ref,
    counts_ref,
    pixels_ref,
    gain_ref,
    bias_ref,
    query_ref,
    table,
    embed,
    key_block,
    wout,
    value_all,
    fold_all,
    rows_f32,
    rows_all,
    coeff_all,
    basis,
    mix_send,
    mix_recv,
    local_sem,
    value_ss,
    value_rs,
    fold_ss,
    fold_rs,
    rows_ss,
    rows_rs,
    coeff_ss,
    coeff_rs,
    mix_ss,
    mix_rs,
):
    n, nv, groups, slots, taps, patches, width, heads, head_size = dims
    padded = rows_f32.shape[1]
    depth = key_block.shape[0]
    columns = key_block.shape[1]
    local_heads = heads // groups
    half = patches * groups // nv
    owned = patches // nv
    basis_rows = nv * (taps + 2) * padded

    b = lax.axis_index("dp")
    v = lax.axis_index("var")
    r, g = v // groups, v % groups
    pair = n % 2 == 0
    lo_size = 2 if pair else 1
    hi_size = n // lo_size
    hi, lo = b // lo_size, b % lo_size

    def remote(src, dst, ss, rs, **where):
        return pltpu.make_async_remote_copy(
            src_ref=src,
            dst_ref=dst,
            send_sem=ss,
            recv_sem=rs,
            device_id=where,
            device_id_type=pl.DeviceIdType.MESH,
        )

    barrier = pltpu.get_barrier_semaphore()
    for off in range(1, n):
        pl.semaphore_signal(
            barrier, inc=1, device_id={"dp": (b + off) % n}, device_id_type=pl.DeviceIdType.MESH
        )
    for off in range(1, nv):
        pl.semaphore_signal(
            barrier, inc=1, device_id={"var": (v + off) % nv}, device_id_type=pl.DeviceIdType.MESH
        )

    mine = pl.ds(pl.multiple_of(g * columns, columns), columns)
    get_query = pltpu.make_async_copy(query_hbm, query_ref, local_sem.at[5])
    get_ids = pltpu.make_async_copy(ids_hbm, ids_ref, local_sem.at[6])
    get_pixels = pltpu.make_async_copy(pixels_hbm, pixels_ref, local_sem.at[7])
    get_gain = pltpu.make_async_copy(gain_hbm, gain_ref, local_sem.at[8])
    get_bias = pltpu.make_async_copy(bias_hbm, bias_ref, local_sem.at[9])
    get_counts = pltpu.make_async_copy(counts_hbm, counts_ref, local_sem.at[10])
    get_key = pltpu.make_async_copy(key_hbm.at[:, mine], key_block, local_sem.at[0])
    get_value = pltpu.make_async_copy(value_hbm.at[:, mine], value_all.at[b], local_sem.at[1])
    get_table = pltpu.make_async_copy(table_hbm, table, local_sem.at[2])
    get_embed = pltpu.make_async_copy(embed_hbm, embed, local_sem.at[3])
    get_out = pltpu.make_async_copy(out_hbm, wout, local_sem.at[4])
    get_value.start()
    get_query.start()
    get_key.start()
    get_ids.start()
    get_pixels.start()
    get_table.start()
    get_embed.start()
    get_gain.start()
    get_bias.start()
    get_counts.start()
    get_out.start()

    fold_rows = fold_all.shape[1]
    get_query.wait()
    pick = (
        lax.broadcasted_iota(jnp.int32, (fold_rows, heads), 1)
        == lax.broadcasted_iota(jnp.int32, (fold_rows, heads), 0) + g * local_heads
    ).astype(F32)
    own_query = jnp.dot(pick, query_ref[...], precision=EXACT, preferred_element_type=F32)
    spread_out = (
        lax.broadcasted_iota(jnp.int32, (head_size, columns), 1) % head_size
        == lax.broadcasted_iota(jnp.int32, (head_size, columns), 0)
    ).astype(F32)
    tiled = jnp.dot(own_query, spread_out, precision=EXACT, preferred_element_type=F32)
    own_head = (
        lax.broadcasted_iota(jnp.int32, (fold_rows, columns), 1) // head_size
        == lax.broadcasted_iota(jnp.int32, (fold_rows, columns), 0)
    )
    diagonal = jnp.where(own_head, tiled, 0.0) * (1.0 / math.sqrt(head_size))

    get_key.wait()
    fold_all[b] = lax.dot_general(
        diagonal,
        key_block[...].astype(F32),
        (((1,), (1,)), ((), ())),
        precision=EXACT,
        preferred_element_type=F32,
    )
    get_value.wait()
    pl.semaphore_wait(barrier, n + nv - 2)

    fold_sends = []
    for off in range(1, n):
        copy = remote(
            fold_all.at[b], fold_all.at[b], fold_ss.at[off], fold_rs.at[off], dp=(b + off) % n
        )
        copy.start()
        fold_sends.append(copy)

    value_sends = []

    def send_value(owner, sem, **where):
        copy = remote(
            value_all.at[owner], value_all.at[owner], value_ss.at[sem], value_rs.at[sem], **where
        )
        copy.start()
        value_sends.append(copy)

    def value_from(owner, sem):
        return remote(
            value_all.at[owner], value_all.at[owner], value_ss.at[sem], value_rs.at[sem], dp=b
        )

    mate = hi * lo_size + (lo_size - 1 - lo)
    if pair:
        send_value(b, hi_size, dp=mate)
    for off in range(1, hi_size):
        send_value(b, off, dp=((hi + off) % hi_size) * lo_size + lo)


    rows_f32[...] = jnp.zeros_like(rows_f32)
    get_ids.wait()
    get_table.wait()
    get_embed.wait()
    slot_of = lax.broadcasted_iota(jnp.int32, (padded, embed.shape[0]), 0)
    wanted = jnp.full((padded, embed.shape[0]), -1, jnp.int32)
    for s in range(slots):
        rows = table[ids_ref[0, s]].astype(F32)
        for k in range(taps):
            rows_f32[k, s : s + 1, :] = rows[k : k + 1, :]
        wanted = jnp.where(slot_of == s, ids_ref[0, s], wanted)
    hot = (wanted == lax.broadcasted_iota(jnp.int32, wanted.shape, 1)).astype(BF16)
    rows_f32[taps] = jnp.dot(hot, embed[...], preferred_element_type=F32)
    rows_all[v] = rows_f32[...].astype(BF16)


    centred = []
    for k in range(taps + 1):
        row = rows_f32[k]
        centred.append(row - jnp.mean(row, axis=-1, keepdims=True))

    rows_sends = []
    for off in range(1, nv):
        copy = remote(
            rows_all.at[v], rows_all.at[v], rows_ss.at[off], rows_rs.at[off], var=(v + off) % nv
        )
        copy.start()
        rows_sends.append(copy)

    get_pixels.wait()
    pix = pixels_ref[0].astype(F32)
    fill = jnp.zeros((padded - slots, patches), F32)
    field = []
    for k in range(taps):
        own = [pix[s, k : k + 1, :] for s in range(slots)]
        field.append(jnp.concatenate(own + ([fill] if padded > slots else []), axis=0))
    field.append(jnp.ones((padded, patches), F32))
    variance = jnp.zeros((padded, patches), F32)
    for k in range(taps + 1):
        for m in range(k, taps + 1):
            gram = jnp.mean(centred[k] * centred[m], axis=-1, keepdims=True)
            variance += (1.0 if m == k else 2.0) * gram * (field[k] * field[m])
    scale = lax.rsqrt(jnp.maximum(variance, 0.0) + 1e-05)
    for k in range(taps + 1):
        coeff_all[v, k] = field[k] * scale

    def forward(off):
        owner = ((hi + hi_size - off) % hi_size) * lo_size + lo
        value_from(owner, off).wait_recv()
        if pair:
            send_value(owner, hi_size + off, dp=mate)

    if hi_size > 1:
        forward(1)
    coeff_sends = []
    for off in range(1, nv):
        copy = remote(
            coeff_all.at[v], coeff_all.at[v], coeff_ss.at[off], coeff_rs.at[off], var=(v + off) % nv
        )
        copy.start()
        coeff_sends.append(copy)
    for off in range(2, hi_size):
        forward(off)

    get_gain.wait()
    get_bias.wait()
    gain = gain_ref[...]
    for off in range(nv):
        src = (v + nv - off) % nv
        if off:
            remote(
                rows_all.at[src], rows_all.at[src], rows_ss.at[off], rows_rs.at[off], var=v
            ).wait_recv()
        for k in range(taps + 1):
            row = rows_all[src, k].astype(F32)
            basis[src, k] = (row - jnp.mean(row, axis=-1, keepdims=True)) * gain
        basis[src, taps + 1] = jnp.broadcast_to(bias_ref[...], (padded, width))

    for off in range(1, n):
        src = (b + n - off) % n
        remote(
            fold_all.at[src], fold_all.at[src], fold_ss.at[off], fold_rs.at[off], dp=b
        ).wait_recv()
    flat = basis[...].reshape(basis_rows, width)
    folded = jnp.concatenate([fold_all[i] for i in range(n)], axis=1)
    score_of = lax.dot_general(
        flat, folded, (((1,), (1,)), ((), ())), precision=EXACT, preferred_element_type=F32
    ).reshape(nv, taps + 2, padded, fold_rows)

    for off in range(1, nv):
        src = (v + nv - off) % nv
        remote(
            coeff_all.at[src], coeff_all.at[src], coeff_ss.at[off], coeff_rs.at[off], var=v
        ).wait_recv()
    get_counts.wait()
    window = pl.ds(pl.multiple_of(r * half, half), half)
    coeff = [coeff_all[:, k, :, window] for k in range(taps + 1)]
    place = lax.broadcasted_iota(jnp.int32, (nv, padded, half), 1)
    slot = lax.broadcasted_iota(jnp.int32, (nv, padded, half), 0) * slots + place
    live = (place < slots) & (slot < counts_ref[0])
    weights = []
    for h in range(local_heads):
        score = jnp.broadcast_to(score_of[:, taps + 1, :, h : h + 1], (nv, padded, half))
        for k in range(taps + 1):
            score = score + coeff[k] * score_of[:, k, :, h : h + 1]
        score = jnp.where(live, score, -1e30)
        peak = jnp.max(jnp.max(score, axis=0, keepdims=True), axis=1, keepdims=True)
        expo = jnp.exp(score - peak)
        total = jnp.sum(jnp.sum(expo, axis=0, keepdims=True), axis=1, keepdims=True)
        prob = expo / total
        parts = [prob * coeff[k] for k in range(taps + 1)] + [prob]
        weights.append(jnp.stack(parts, axis=1).reshape(basis_rows, half).astype(BF16))

    if pair:
        for off in range(hi_size):
            owner = ((hi + hi_size - off) % hi_size) * lo_size + (lo_size - 1 - lo)
            value_from(owner, hi_size + off).wait_recv()
    projected = jnp.dot(
        flat.astype(BF16),
        value_all[...].reshape(width, columns),
        preferred_element_type=F32,
    ).astype(BF16)
    mixed = jnp.concatenate(
        [
            lax.dot_general(
                weights[h],
                projected[:, h * head_size : (h + 1) * head_size],
                (((0,), (0,)), ((), ())),
                preferred_element_type=F32,
            )
            for h in range(local_heads)
        ],
        axis=1,
    ).astype(BF16)
    mix_send[...] = mixed.reshape(groups, owned, columns)

    mix_sends = []
    for off in range(1, groups):
        to = (g + off) % groups
        copy = remote(
            mix_send.at[to], mix_recv.at[g], mix_ss.at[off], mix_rs.at[off], var=r * groups + to
        )
        copy.start()
        mix_sends.append(copy)

    get_out.wait()
    total = jnp.dot(mix_send[g], wout[mine, :], preferred_element_type=F32)
    for off in range(1, groups):
        src = (g + groups - off) % groups
        remote(
            mix_send.at[src], mix_recv.at[src], mix_ss.at[off], mix_rs.at[off], var=v
        ).wait_recv()
        there = pl.ds(pl.multiple_of(src * columns, columns), columns)
        total += jnp.dot(mix_recv[src], wout[there, :], preferred_element_type=F32)
    result_ref[0] = total.astype(result_ref.dtype)

    for copy in value_sends + fold_sends + rows_sends + coeff_sends + mix_sends:
        copy.wait_send()


def on_device(
    n,
    nv,
    pixels,
    var_ids,
    counts,
    patch_weight,
    var_embed,
    norm_gain,
    norm_bias,
    key_weight,
    value_weight,
    query,
    out_weight,
):
    slots, taps, patches = pixels.shape[1:]
    width = out_weight.shape[0]
    heads, head_size = query.shape
    groups = min(nv, width // 128)
    columns = width // groups
    depth = value_weight.shape[0]
    padded = rounded_up(slots, 8)
    owned = patches // nv
    fold_rows = rounded_up(heads // groups, 8)
    vmem = pl.BlockSpec(memory_space=pltpu.VMEM)
    hbm = pl.BlockSpec(memory_space=pl.ANY)
    dims = (n, nv, groups, slots, taps, patches, width, heads, head_size)
    dma = pltpu.SemaphoreType.DMA
    return pl.pallas_call(
        functools.partial(kernel, dims),
        out_shape=pltpu.VMEM((1, owned, width), BF16),
        in_specs=[pl.BlockSpec(memory_space=pltpu.HBM)] * 11,
        out_specs=vmem,
        scratch_shapes=[
            pltpu.SMEM(var_ids.shape, jnp.int32),
            pltpu.SMEM(counts.shape, jnp.int32),
            pltpu.VMEM(pixels.shape, BF16),
            pltpu.VMEM((1, width), F32),
            pltpu.VMEM((1, width), F32),
            pltpu.VMEM(query.shape, F32),
            pltpu.VMEM(patch_weight.shape, BF16),
            pltpu.VMEM(var_embed.shape, BF16),
            pltpu.VMEM((depth, columns), BF16),
            pltpu.VMEM((width, width), BF16),
            pltpu.VMEM((n, depth, columns), BF16),
            pltpu.VMEM((n, fold_rows, depth), F32),
            pltpu.VMEM((taps + 1, padded, width), F32),
            pltpu.VMEM((nv, taps + 1, padded, width), BF16),
            pltpu.VMEM((nv, taps + 1, padded, patches), F32),
            pltpu.VMEM((nv, taps + 2, padded, width), F32),
            pltpu.VMEM((groups, owned, columns), BF16),
            pltpu.VMEM((groups, owned, columns), BF16),
            dma((11,)),
            dma((n,)),
            dma((n,)),
            dma((n,)),
            dma((n,)),
            dma((nv,)),
            dma((nv,)),
            dma((nv,)),
            dma((nv,)),
            dma((groups,)),
            dma((groups,)),
        ],
        compiler_params=pltpu.CompilerParams(collective_id=0, has_side_effects=True),
    )(
        var_ids,
        counts,
        pixels,
        patch_weight,
        var_embed,
        norm_gain.reshape(1, width),
        norm_bias.reshape(1, width),
        key_weight,
        value_weight,
        query,
        out_weight,
    )


def solution(mesh):
    placed = (
        P("dp", "var", None, None),
        P("dp", "var"),
        P("dp"),
        P(),
        P(),
        P(),
        P(),
        P("dp", None),
        P("dp", None),
        P(),
        P(),
    )
    return jax.shard_map(
        functools.partial(on_device, mesh.shape["dp"], mesh.shape["var"]),
        mesh=mesh,
        in_specs=placed,
        out_specs=P("dp", "var", None),
        check_vma=False,
    )
```

```python
import functools
import math

import jax
import jax.numpy as jnp
from jax import lax
from jax.experimental import pallas as pl
from jax.experimental.pallas import tpu as pltpu
from jax.sharding import PartitionSpec as P

F32 = jnp.float32
BF16 = jnp.bfloat16
MESH = pl.DeviceIdType.MESH
PIECES = 3


def rounded_up(value, unit):
    return -(-value // unit) * unit


def flipped(index, bits):
    bit = 1
    while bit <= bits:
        if bits & bit:
            index = index + bit - 2 * bit * ((index // bit) % 2)
        bit *= 2
    return index


def pieces_of(value):
    parts = []
    for _ in range(PIECES):
        part = value.astype(BF16).astype(F32)
        parts.append(part)
        value = value - part
    return parts


def kernel(
    dims,
    pixels_hbm,
    ids_hbm,
    counts_hbm,
    table_hbm,
    embed_hbm,
    gain_hbm,
    bias_hbm,
    key_hbm,
    value_hbm,
    query_hbm,
    out_hbm,
    result_ref,
    ids_all,
    counts_ref,
    pix_all,
    table,
    embed,
    gain_ref,
    bias_ref,
    query_ref,
    key_block,
    value_all,
    wout,
    fold_all,
    own_rows,
    raw,
    left,
    field_ref,
    scale_all,
    scale_ref,
    weight_ref,
    mix_send,
    mix_recv,
    local_sem,
    send_sem,
    once_sem,
    value_rs,
    mix_rs,
):
    n, nv, groups, lo_size, slots, taps, patches, width, heads, head_size = dims
    hi_size = n // lo_size
    team = lo_size * nv
    mixers = lo_size * groups
    depth = key_block.shape[0]
    columns = key_block.shape[1]
    local_heads = heads // groups
    fold_rows = fold_all.shape[1]
    half = patches * groups // nv
    owned = patches // nv
    padded = own_rows.shape[1]
    every = nv * slots
    tap_rows = every * taps
    rows = raw.shape[1]
    tail = rows - tap_rows - every

    b = lax.axis_index("dp")
    v = lax.axis_index("var")
    hi, lo = b // lo_size, b % lo_size
    r, g = v // groups, v % groups
    me = lo * nv + v
    mixer = lo * groups + g

    def mate(bits):
        there = flipped(me, bits)
        return {"dp": hi * lo_size + there // nv, "var": there % nv}

    def remote(src, dst, ss, rs, where):
        return pltpu.make_async_remote_copy(
            src_ref=src, dst_ref=dst, send_sem=ss, recv_sem=rs, device_id=where, device_id_type=MESH
        )

    here = {"dp": b, "var": v}
    barrier = pltpu.get_barrier_semaphore()
    greeted = 0
    for off in range(1, n):
        pl.semaphore_signal(barrier, inc=1, device_id={"dp": (b + off) % n}, device_id_type=MESH)
        greeted += 1
    for bits in range(1, team):
        if bits % nv:
            pl.semaphore_signal(barrier, inc=1, device_id=mate(bits), device_id_type=MESH)
            greeted += 1

    mine = pl.ds(pl.multiple_of(g * columns, columns), columns)
    copies = [
        (query_hbm, query_ref),
        (key_hbm.at[:, mine], key_block),
        (value_hbm.at[:, mine], value_all.at[hi]),
        (ids_hbm, ids_all.at[me]),
        (pixels_hbm.at[0], pix_all.at[me]),
        (table_hbm, table),
        (embed_hbm, embed),
        (gain_hbm, gain_ref),
        (bias_hbm, bias_ref),
        (counts_hbm, counts_ref),
        (out_hbm, wout),
    ]
    gets = [pltpu.make_async_copy(s, d, local_sem.at[i]) for i, (s, d) in enumerate(copies)]
    for get in gets:
        get.start()
    (
        get_query,
        get_key,
        get_value,
        get_ids,
        get_pixels,
        get_table,
        get_embed,
        get_gain,
        get_bias,
        get_counts,
        get_out,
    ) = gets

    get_query.wait()
    own_query = query_ref[:local_heads]
    for i in range(1, groups):
        own_query = jnp.where(
            g == i, query_ref[i * local_heads : (i + 1) * local_heads], own_query
        )
    own_query = own_query * (1.0 / math.sqrt(head_size))
    if fold_rows > local_heads:
        blank = jnp.zeros((fold_rows - local_heads, head_size), F32)
        own_query = jnp.concatenate([own_query, blank], axis=0)
    own_head = (
        lax.broadcasted_iota(jnp.int32, (fold_rows, columns), 1) // head_size
        == lax.broadcasted_iota(jnp.int32, (fold_rows, columns), 0)
    )
    diagonal = jnp.where(own_head, jnp.concatenate([own_query] * local_heads, axis=1), 0.0)
    diagonal = jnp.concatenate(pieces_of(diagonal), axis=0).astype(BF16)
    get_key.wait()
    found = lax.dot_general(
        diagonal, key_block[...], (((1,), (1,)), ((), ())), preferred_element_type=F32
    )
    fold = found[:fold_rows]
    for i in range(1, PIECES):
        fold = fold + found[i * fold_rows : (i + 1) * fold_rows]
    fold_all[b] = fold

    get_value.wait()
    get_pixels.wait()
    get_ids.wait()
    pl.semaphore_wait(barrier, greeted)

    for bits in range(team - 1, 0, -1):
        remote(ids_all.at[me], ids_all.at[me], send_sem.at[0], once_sem.at[0], mate(bits)).start()
        remote(pix_all.at[me], pix_all.at[me], send_sem.at[1], once_sem.at[1], mate(bits)).start()
    for off in range(1, n):
        there = {"dp": (b + off) % n}
        remote(fold_all.at[b], fold_all.at[b], send_sem.at[3], once_sem.at[2], there).start()
    ring = sorted(range(1, hi_size), key=lambda off: -min(off, hi_size - off))
    for off in ring:
        there = {"dp": ((hi + off) % hi_size) * lo_size + lo}
        remote(value_all.at[hi], value_all.at[hi], send_sem.at[2], value_rs.at[off], there).start()

    get_table.wait()
    get_embed.wait()
    own_rows[...] = jnp.zeros_like(own_rows)
    ids_at = lax.broadcasted_iota(jnp.int32, (padded, embed.shape[0]), 0)
    wanted = jnp.full((padded, embed.shape[0]), -1, jnp.int32)
    for s in range(slots):
        chosen = ids_all[me, 0, s]
        found = table[chosen].astype(F32)
        for k in range(taps):
            own_rows[k, s : s + 1, :] = found[k : k + 1, :]
        wanted = jnp.where(ids_at == s, chosen, wanted)
    hot = (wanted == lax.broadcasted_iota(jnp.int32, wanted.shape, 1)).astype(BF16)
    own_rows[taps] = jnp.dot(hot, embed[...], preferred_element_type=F32)
    centred = []
    for k in range(taps + 1):
        row = own_rows[k]
        centred.append(row - jnp.mean(row, axis=-1, keepdims=True))
    pix = pix_all[me].astype(F32)
    fill = jnp.zeros((padded - slots, patches), F32)
    field = []
    for k in range(taps):
        own = [pix[s, k : k + 1, :] for s in range(slots)]
        field.append(jnp.concatenate(own + ([fill] if padded > slots else []), axis=0))
    field.append(jnp.ones((padded, patches), F32))
    variance = jnp.zeros((padded, patches), F32)
    for k in range(taps + 1):
        for m in range(k, taps + 1):
            gram = jnp.mean(centred[k] * centred[m], axis=-1, keepdims=True)
            variance += (1.0 if m == k else 2.0) * gram * (field[k] * field[m])
    scale = lax.rsqrt(jnp.maximum(variance, 0.0) + 1e-05)
    get_counts.wait()
    place = lax.broadcasted_iota(jnp.int32, (padded, patches), 0)
    live = (place < slots) & (v * slots + place < counts_ref[0])
    scale_all[me] = jnp.where(live, scale, -1.0)
    for bits in range(team - 1, 0, -1):
        remote(
            scale_all.at[me], scale_all.at[me], send_sem.at[4], once_sem.at[3], mate(bits)
        ).start()

    def arrived(ref, count, ss, rs):
        block = ref.at[pl.ds(0, count)]
        return remote(block, block, ss, rs, here)

    all_ids = arrived(ids_all, team - 1, send_sem.at[0], once_sem.at[0])
    all_ids.wait_recv()
    get_gain.wait()
    get_bias.wait()
    gain = gain_ref[...]
    slot_at = lax.broadcasted_iota(jnp.int32, (every, embed.shape[0]), 0)
    for j in range(lo_size):
        wanted = jnp.full((every, embed.shape[0]), -1, jnp.int32)
        for s in range(every):
            chosen = ids_all[j * nv + s // slots, 0, s % slots]
            raw[j, s * taps : (s + 1) * taps, :] = table[chosen].astype(F32)
            wanted = jnp.where(slot_at == s, chosen, wanted)
        hot = (wanted == lax.broadcasted_iota(jnp.int32, wanted.shape, 1)).astype(BF16)
        raw[j, tap_rows : tap_rows + every, :] = jnp.dot(
            hot, embed[...], preferred_element_type=F32
        )
        raw[j, tap_rows + every :, :] = jnp.zeros((tail, width), F32)
        row = raw[j, : tap_rows + every, :]
        row = (row - jnp.mean(row, axis=-1, keepdims=True)) * gain
        last = lax.broadcasted_iota(jnp.int32, (tail, width), 0)
        last = jnp.where(last == 0, bias_ref[...], 0.0)
        basis = jnp.concatenate([row, last], axis=0)
        for h in range(hi_size):
            at = h * lo_size * depth
            part = basis[:, at : at + depth]
            for other in range(1, lo_size):
                at += depth
                part = jnp.where(lo == other, basis[:, at : at + depth], part)
            left[h, j * rows : (j + 1) * rows, :] = part.astype(BF16)

    all_folds = arrived(fold_all, n - 1, send_sem.at[3], once_sem.at[2])
    all_folds.wait_recv()
    folded = jnp.concatenate([fold_all[i] for i in range(n)], axis=1)
    bias_score = jnp.sum(folded * bias_ref[...], axis=-1, keepdims=True)
    folded = folded * gain
    fold_sum = jnp.sum(folded, axis=-1, keepdims=True)
    keys = jnp.concatenate(pieces_of(folded) + [jnp.ones((8, width), F32)], axis=0).astype(BF16)

    all_pixels = arrived(pix_all, team - 1, send_sem.at[1], once_sem.at[1])
    all_pixels.wait_recv()
    all_scales = arrived(scale_all, team - 1, send_sem.at[4], once_sem.at[3])
    all_scales.wait_recv()
    window = pl.ds(pl.multiple_of(r * half, half), half)

    which = lax.broadcasted_iota(jnp.int32, (every, rows), 0)
    what = lax.broadcasted_iota(jnp.int32, (every, rows), 1)
    of_slot = jnp.where(what < tap_rows, what // taps, what - tap_rows) == which
    to_row = lax.broadcasted_iota(jnp.int32, (rows, every + 8), 0)
    of_row = jnp.where(to_row < tap_rows, to_row // taps, to_row - tap_rows)
    widen = (of_row == lax.broadcasted_iota(jnp.int32, (rows, every + 8), 1)).astype(BF16)

    for j in range(lo_size):
        for s in range(every):
            field_ref[s * taps : (s + 1) * taps, :] = pix_all[
                j * nv + s // slots, s % slots, :, window
            ].astype(F32)
        for i in range(nv):
            scale_ref[i * slots : (i + 1) * slots, :] = scale_all[j * nv + i, :slots, window]
        field_ref[tap_rows:, :] = jnp.ones((rows - tap_rows, half), F32)
        field = field_ref[...]
        scale = scale_ref[...]
        live = scale > 0.0

        found = lax.dot_general(
            keys, raw[j].astype(BF16), (((1,), (1,)), ((), ())), preferred_element_type=F32
        )
        score_of = found[:fold_rows]
        for i in range(1, PIECES):
            score_of = score_of + found[i * fold_rows : (i + 1) * fold_rows]
        row_sum = found[PIECES * fold_rows : PIECES * fold_rows + 1]
        score_of = score_of - (row_sum * (1.0 / width)) * fold_sum
        blocks = [
            jnp.where(of_slot, part[h : h + 1, :], 0.0)
            for h in range(local_heads)
            for part in pieces_of(score_of)
        ]
        slot_scores = jnp.dot(
            jnp.concatenate(blocks, axis=0).astype(BF16),
            field.astype(BF16),
            preferred_element_type=F32,
        )
        shares = []
        for h in range(local_heads):
            first = h * PIECES * every
            score = slot_scores[first : first + every]
            for i in range(1, PIECES):
                first += every
                score = score + slot_scores[first : first + every]
            score = score * scale + bias_score[h : h + 1, :]
            score = jnp.where(live, score, -1e30)
            expo = jnp.exp(score - jnp.max(score, axis=0, keepdims=True))
            prob = expo * (1.0 / jnp.sum(expo, axis=0, keepdims=True))
            whole = jnp.broadcast_to(jnp.sum(prob, axis=0, keepdims=True), (8, half))
            shares.append(jnp.concatenate([prob * scale, whole], axis=0))
        wide = jnp.dot(
            widen, jnp.concatenate(shares, axis=1).astype(BF16), preferred_element_type=F32
        )
        for h in range(local_heads):
            weight = wide[:, h * half : (h + 1) * half] * field
            weight_ref[j, :, h * rows : (h + 1) * rows] = weight.T.astype(BF16)

    projected = jnp.dot(left[hi], value_all[hi], preferred_element_type=F32)
    for off in ring[::-1]:
        src = (hi + hi_size - off) % hi_size
        remote(
            value_all.at[src], value_all.at[src], send_sem.at[2], value_rs.at[off], here
        ).wait_recv()
        projected += jnp.dot(left[src], value_all[src], preferred_element_type=F32)

    of_column = lax.broadcasted_iota(jnp.int32, (rows, columns), 1) // head_size
    for j in range(lo_size):
        part = projected[j * rows : (j + 1) * rows]
        spread = jnp.concatenate(
            [jnp.where(of_column == h, part, 0.0) for h in range(local_heads)], axis=0
        ).astype(BF16)
        mixed = jnp.dot(weight_ref[j], spread, preferred_element_type=F32).astype(BF16)
        mix_send[j * groups : (j + 1) * groups] = mixed.reshape(groups, owned, columns)

    for bits in range(mixers - 1, 0, -1):
        to = flipped(mixer, bits)
        there = {"dp": hi * lo_size + to // groups, "var": r * groups + to % groups}
        remote(
            mix_send.at[to], mix_recv.at[mixer], send_sem.at[5], mix_rs.at[bits], there
        ).start()

    get_out.wait()
    total = jnp.zeros((owned, width), F32)
    for near in range(groups):
        summed = None
        for far in range(lo_size):
            bits = far * groups + near
            src = flipped(mixer, bits)
            if bits:
                remote(
                    mix_send.at[src], mix_recv.at[src], send_sem.at[5], mix_rs.at[bits], here
                ).wait_recv()
                part = mix_recv[src].astype(F32)
            else:
                part = mix_send[src].astype(F32)
            summed = part if summed is None else summed + part
        there = pl.ds(pl.multiple_of(flipped(g, near) * columns, columns), columns)
        total += jnp.dot(summed.astype(BF16), wout[there, :], preferred_element_type=F32)
    result_ref[0] = total.astype(result_ref.dtype)

    all_ids.wait_send()
    all_pixels.wait_send()
    all_folds.wait_send()
    all_scales.wait_send()
    arrived(value_all, hi_size - 1, send_sem.at[2], value_rs.at[0]).wait_send()
    arrived(mix_send, mixers - 1, send_sem.at[5], mix_rs.at[0]).wait_send()


def on_device(
    n,
    nv,
    pixels,
    var_ids,
    counts,
    patch_weight,
    var_embed,
    norm_gain,
    norm_bias,
    key_weight,
    value_weight,
    query,
    out_weight,
):
    slots, taps, patches = pixels.shape[1:]
    width = out_weight.shape[0]
    heads, head_size = query.shape
    groups = min(nv, width // 128)
    lo_size = 2 if n % 2 == 0 else 1
    hi_size = n // lo_size
    team = lo_size * nv
    mixers = lo_size * groups
    columns = width // groups
    depth = value_weight.shape[0]
    padded = rounded_up(slots, 8)
    owned = patches // nv
    half = patches * groups // nv
    local_heads = heads // groups
    fold_rows = rounded_up(local_heads, 8)
    every = nv * slots
    rows = rounded_up(every * taps + every + 1, 16)
    hbm = pl.BlockSpec(memory_space=pltpu.HBM)
    vmem = pl.BlockSpec(memory_space=pltpu.VMEM)
    dims = (n, nv, groups, lo_size, slots, taps, patches, width, heads, head_size)
    dma = pltpu.SemaphoreType.DMA
    return pl.pallas_call(
        functools.partial(kernel, dims),
        out_shape=pltpu.VMEM((1, owned, width), BF16),
        in_specs=[hbm] * 11,
        out_specs=vmem,
        scratch_shapes=[
            pltpu.SMEM((team,) + var_ids.shape, jnp.int32),
            pltpu.SMEM(counts.shape, jnp.int32),
            pltpu.VMEM((team, slots, taps, patches), BF16),
            pltpu.VMEM(patch_weight.shape, BF16),
            pltpu.VMEM(var_embed.shape, BF16),
            pltpu.VMEM((1, width), F32),
            pltpu.VMEM((1, width), F32),
            pltpu.VMEM(query.shape, F32),
            pltpu.VMEM((depth, columns), BF16),
            pltpu.VMEM((hi_size, depth, columns), BF16),
            pltpu.VMEM((width, width), BF16),
            pltpu.VMEM((n, fold_rows, depth), F32),
            pltpu.VMEM((taps + 1, padded, width), F32),
            pltpu.VMEM((lo_size, rows, width), F32),
            pltpu.VMEM((hi_size, lo_size * rows, depth), BF16),
            pltpu.VMEM((rows, half), F32),
            pltpu.VMEM((team, padded, patches), F32),
            pltpu.VMEM((every, half), F32),
            pltpu.VMEM((lo_size, half, local_heads * rows), BF16),
            pltpu.VMEM((mixers, owned, columns), BF16),
            pltpu.VMEM((mixers, owned, columns), BF16),
            dma((11,)),
            dma((6,)),
            dma((4,)),
            dma((hi_size,)),
            dma((mixers,)),
        ],
        compiler_params=pltpu.CompilerParams(collective_id=0, has_side_effects=True),
    )(
        pixels,
        var_ids,
        counts,
        patch_weight,
        var_embed,
        norm_gain.reshape(1, width),
        norm_bias.reshape(1, width),
        key_weight,
        value_weight,
        query,
        out_weight,
    )


def solution(mesh):
    placed = (
        P("dp", "var", None, None),
        P("dp", "var"),
        P("dp"),
        P(),
        P(),
        P(),
        P(),
        P("dp", None),
        P("dp", None),
        P(),
        P(),
    )
    return jax.shard_map(
        functools.partial(on_device, mesh.shape["dp"], mesh.shape["var"]),
        mesh=mesh,
        in_specs=placed,
        out_specs=P("dp", "var", None),
        check_vma=False,
    )
```

```python
import functools
import math

import jax
import jax.numpy as jnp
from jax import lax
from jax.experimental import pallas as pl
from jax.experimental.pallas import tpu as pltpu
from jax.sharding import PartitionSpec as P

F32 = jnp.float32
BF16 = jnp.bfloat16
MESH = pl.DeviceIdType.MESH
PIECES = 3


def rounded_up(value, unit):
    return -(-value // unit) * unit


def flipped(index, bits):
    bit = 1
    while bit <= bits:
        if bits & bit:
            index = index + bit - 2 * bit * ((index // bit) % 2)
        bit *= 2
    return index


def pieces_of(value):
    parts = []
    for _ in range(PIECES):
        part = value.astype(BF16).astype(F32)
        parts.append(part)
        value = value - part
    return parts


def kernel(
    dims,
    pixels_hbm,
    ids_hbm,
    counts_hbm,
    table_hbm,
    embed_hbm,
    gain_hbm,
    bias_hbm,
    key_hbm,
    value_hbm,
    query_hbm,
    out_hbm,
    result_ref,
    ids_all,
    counts_ref,
    pix_all,
    table,
    embed,
    gain_ref,
    bias_ref,
    query_ref,
    key_block,
    value_send,
    value_all,
    wout,
    fold_all,
    own_rows,
    raw,
    left,
    field_ref,
    scale_all,
    scale_ref,
    score_ref,
    weight_ref,
    mix_send,
    mix_recv,
    local_sem,
    send_sem,
    once_sem,
    value_rs,
    mix_rs,
):
    n, nv, groups, lo_size, slots, taps, patches, width, heads, head_size = dims
    hi_size = n // lo_size
    team = lo_size * nv
    mixers = lo_size * groups
    depth = key_block.shape[0]
    columns = key_block.shape[1]
    halves = value_all.shape[0]
    strip = columns // halves
    crossed = groups % 2 == 0
    local_heads = heads // groups
    fold_rows = fold_all.shape[1]
    half = patches * groups // nv
    owned = patches // nv
    padded = own_rows.shape[1]
    every = nv * slots
    tap_rows = every * taps
    rows = raw.shape[1]
    tail = rows - tap_rows - every

    b = lax.axis_index("dp")
    v = lax.axis_index("var")
    hi, lo = b // lo_size, b % lo_size
    r, g = v // groups, v % groups
    me = lo * nv + v
    mixer = lo * groups + g

    def mate(bits):
        there = flipped(me, bits)
        return {"dp": hi * lo_size + there // nv, "var": there % nv}

    def remote(src, dst, ss, rs, where):
        return pltpu.make_async_remote_copy(
            src_ref=src, dst_ref=dst, send_sem=ss, recv_sem=rs, device_id=where, device_id_type=MESH
        )

    here = {"dp": b, "var": v}
    barrier = pltpu.get_barrier_semaphore()
    greeted = 0
    for off in range(1, n):
        pl.semaphore_signal(barrier, inc=1, device_id={"dp": (b + off) % n}, device_id_type=MESH)
        greeted += 1
    for bits in range(1, team):
        if bits % nv:
            pl.semaphore_signal(barrier, inc=1, device_id=mate(bits), device_id_type=MESH)
            greeted += 1

    if crossed:
        for off in range(1, hi_size):
            there = {"dp": ((hi + off) % hi_size) * lo_size + lo, "var": flipped(v, 1)}
            pl.semaphore_signal(barrier, inc=1, device_id=there, device_id_type=MESH)
            greeted += 1
    to_core = flipped(v, 1) if crossed else v
    to_group = flipped(g, 1) if crossed else g

    mine = pl.ds(pl.multiple_of(g * columns, columns), columns)

    def strip_of(group, a):
        return pl.ds(pl.multiple_of(group * columns + a * strip, strip), strip)

    copies = [
        (query_hbm, query_ref),
        (key_hbm.at[:, mine], key_block),
        (ids_hbm, ids_all.at[me]),
        (pixels_hbm.at[0], pix_all.at[me]),
        (table_hbm, table),
        (embed_hbm, embed),
        (gain_hbm, gain_ref),
        (bias_hbm, bias_ref),
        (counts_hbm, counts_ref),
        (out_hbm, wout),
    ]
    copies += [(value_hbm.at[:, strip_of(g, a)], value_all.at[a, hi]) for a in range(halves)]
    copies[2:2] = [
        (value_hbm.at[:, strip_of(to_group, a)], value_send.at[a]) for a in range(halves)
    ]
    gets = [pltpu.make_async_copy(s, d, local_sem.at[i]) for i, (s, d) in enumerate(copies)]
    for get in gets:
        get.start()
    get_query, get_key = gets[:2]
    get_strips = gets[2 : 2 + halves]
    get_values = gets[-halves:]
    (
        get_ids,
        get_pixels,
        get_table,
        get_embed,
        get_gain,
        get_bias,
        get_counts,
        get_out,
    ) = gets[2 + halves : -halves]

    get_query.wait()
    own_query = query_ref[:local_heads]
    for i in range(1, groups):
        own_query = jnp.where(
            g == i, query_ref[i * local_heads : (i + 1) * local_heads], own_query
        )
    own_query = own_query * (1.0 / math.sqrt(head_size))
    if fold_rows > local_heads:
        blank = jnp.zeros((fold_rows - local_heads, head_size), F32)
        own_query = jnp.concatenate([own_query, blank], axis=0)
    own_head = (
        lax.broadcasted_iota(jnp.int32, (fold_rows, columns), 1) // head_size
        == lax.broadcasted_iota(jnp.int32, (fold_rows, columns), 0)
    )
    diagonal = jnp.where(own_head, jnp.concatenate([own_query] * local_heads, axis=1), 0.0)
    diagonal = jnp.concatenate(pieces_of(diagonal), axis=0).astype(BF16)
    get_key.wait()
    found = lax.dot_general(
        diagonal, key_block[...], (((1,), (1,)), ((), ())), preferred_element_type=F32
    )
    fold = found[:fold_rows]
    for i in range(1, PIECES):
        fold = fold + found[i * fold_rows : (i + 1) * fold_rows]
    fold_all[b] = fold

    get_ids.wait()
    get_pixels.wait()
    get_table.wait()
    get_embed.wait()
    own_rows[...] = jnp.zeros_like(own_rows)
    ids_at = lax.broadcasted_iota(jnp.int32, (padded, embed.shape[0]), 0)
    wanted = jnp.full((padded, embed.shape[0]), -1, jnp.int32)
    for s in range(slots):
        chosen = ids_all[me, 0, s]
        found = table[chosen].astype(F32)
        for k in range(taps):
            own_rows[k, s : s + 1, :] = found[k : k + 1, :]
        wanted = jnp.where(ids_at == s, chosen, wanted)
    hot = (wanted == lax.broadcasted_iota(jnp.int32, wanted.shape, 1)).astype(BF16)
    own_rows[taps] = jnp.dot(hot, embed[...], preferred_element_type=F32)
    centred = []
    for k in range(taps + 1):
        row = own_rows[k]
        centred.append(row - jnp.mean(row, axis=-1, keepdims=True))
    pix = pix_all[me].astype(F32)
    fill = jnp.zeros((padded - slots, patches), F32)
    field = []
    for k in range(taps):
        own = [pix[s, k : k + 1, :] for s in range(slots)]
        field.append(jnp.concatenate(own + ([fill] if padded > slots else []), axis=0))
    field.append(jnp.ones((padded, patches), F32))
    variance = jnp.zeros((padded, patches), F32)
    for k in range(taps + 1):
        for m in range(k, taps + 1):
            gram = jnp.mean(centred[k] * centred[m], axis=-1, keepdims=True)
            variance += (1.0 if m == k else 2.0) * gram * (field[k] * field[m])
    scale = lax.rsqrt(jnp.maximum(variance, 0.0) + 1e-05)
    get_counts.wait()
    place = lax.broadcasted_iota(jnp.int32, (padded, patches), 0)
    live = (place < slots) & (v * slots + place < counts_ref[0])
    scale_all[me] = jnp.where(live, scale, -1.0)
    for get in get_strips:
        get.wait()
    pl.semaphore_wait(barrier, greeted)

    for bits in range(team - 1, 0, -1):
        remote(ids_all.at[me], ids_all.at[me], send_sem.at[0], once_sem.at[0], mate(bits)).start()
        remote(pix_all.at[me], pix_all.at[me], send_sem.at[1], once_sem.at[1], mate(bits)).start()
    for bits in range(team - 1, 0, -1):
        remote(
            scale_all.at[me], scale_all.at[me], send_sem.at[4], once_sem.at[3], mate(bits)
        ).start()
    for off in range(1, n):
        there = {"dp": (b + off) % n}
        remote(fold_all.at[b], fold_all.at[b], send_sem.at[3], once_sem.at[2], there).start()
    ring = sorted(range(1, hi_size), key=lambda off: -min(off, hi_size - off))
    for a in range(halves):
        for off in ring:
            there = {"dp": ((hi + off) % hi_size) * lo_size + lo, "var": to_core}
            remote(
                value_send.at[a], value_all.at[a, hi], send_sem.at[2], value_rs.at[a, off], there
            ).start()

    def arrived(ref, count, ss, rs):
        block = ref.at[pl.ds(0, count)]
        return remote(block, block, ss, rs, here)

    all_ids = arrived(ids_all, team - 1, send_sem.at[0], once_sem.at[0])
    all_ids.wait_recv()
    get_gain.wait()
    get_bias.wait()
    gain = gain_ref[...]
    slot_at = lax.broadcasted_iota(jnp.int32, (every, embed.shape[0]), 0)
    for j in range(lo_size):
        wanted = jnp.full((every, embed.shape[0]), -1, jnp.int32)
        for s in range(every):
            chosen = ids_all[j * nv + s // slots, 0, s % slots]
            raw[j, s * taps : (s + 1) * taps, :] = table[chosen].astype(F32)
            wanted = jnp.where(slot_at == s, chosen, wanted)
        hot = (wanted == lax.broadcasted_iota(jnp.int32, wanted.shape, 1)).astype(BF16)
        raw[j, tap_rows : tap_rows + every, :] = jnp.dot(
            hot, embed[...], preferred_element_type=F32
        )
        raw[j, tap_rows + every :, :] = jnp.zeros((tail, width), F32)
        row = raw[j, : tap_rows + every, :]
        row = (row - jnp.mean(row, axis=-1, keepdims=True)) * gain
        last = lax.broadcasted_iota(jnp.int32, (tail, width), 0)
        last = jnp.where(last == 0, bias_ref[...], 0.0)
        basis = jnp.concatenate([row, last], axis=0)
        for h in range(hi_size):
            at = h * lo_size * depth
            part = basis[:, at : at + depth]
            for other in range(1, lo_size):
                at += depth
                part = jnp.where(lo == other, basis[:, at : at + depth], part)
            left[h, j * rows : (j + 1) * rows, :] = part.astype(BF16)

    all_folds = arrived(fold_all, n - 1, send_sem.at[3], once_sem.at[2])
    all_folds.wait_recv()
    folded = jnp.concatenate([fold_all[i] for i in range(n)], axis=1)
    bias_score = jnp.sum(folded * bias_ref[...], axis=-1, keepdims=True)
    folded = folded * gain
    fold_sum = jnp.sum(folded, axis=-1, keepdims=True)
    keys = jnp.concatenate(pieces_of(folded) + [jnp.ones((8, width), F32)], axis=0).astype(BF16)

    which = lax.broadcasted_iota(jnp.int32, (every, rows), 0)
    what = lax.broadcasted_iota(jnp.int32, (every, rows), 1)
    of_slot = jnp.where(what < tap_rows, what // taps, what - tap_rows) == which
    to_row = lax.broadcasted_iota(jnp.int32, (rows, every + 8), 0)
    of_row = jnp.where(to_row < tap_rows, to_row // taps, to_row - tap_rows)
    widen = (of_row == lax.broadcasted_iota(jnp.int32, (rows, every + 8), 1)).astype(BF16)

    blocks = []
    for j in range(lo_size):
        found = lax.dot_general(
            keys, raw[j].astype(BF16), (((1,), (1,)), ((), ())), preferred_element_type=F32
        )
        score_of = found[:fold_rows]
        for i in range(1, PIECES):
            score_of = score_of + found[i * fold_rows : (i + 1) * fold_rows]
        row_sum = found[PIECES * fold_rows : PIECES * fold_rows + 1]
        score_of = score_of - (row_sum * (1.0 / width)) * fold_sum
        parts = [
            jnp.where(of_slot, part[h : h + 1, :], 0.0)
            for part in pieces_of(score_of)
            for h in range(local_heads)
        ]
        blocks.append(jnp.concatenate(parts, axis=0).astype(BF16))

    all_pixels = arrived(pix_all, team - 1, send_sem.at[1], once_sem.at[1])
    all_pixels.wait_recv()
    window = pl.ds(pl.multiple_of(r * half, half), half)
    for j in range(lo_size):
        for s in range(every):
            field_ref[j, s * taps : (s + 1) * taps, :] = pix_all[
                j * nv + s // slots, s % slots, :, window
            ].astype(F32)
        field_ref[j, tap_rows:, :] = jnp.ones((rows - tap_rows, half), F32)
        found = jnp.dot(blocks[j], field_ref[j].astype(BF16), preferred_element_type=F32)
        every_head = local_heads * every
        score = found[:every_head]
        for i in range(1, PIECES):
            score = score + found[i * every_head : (i + 1) * every_head]
        score_ref[j] = score

    all_scales = arrived(scale_all, team - 1, send_sem.at[4], once_sem.at[3])
    all_scales.wait_recv()
    for j in range(lo_size):
        for i in range(nv):
            scale_ref[j, i * slots : (i + 1) * slots, :] = scale_all[j * nv + i, :slots, window]
        scale = scale_ref[j]
        live = scale > 0.0
        shares = []
        for h in range(local_heads):
            score = score_ref[j, h * every : (h + 1) * every, :]
            score = score * scale + bias_score[h : h + 1, :]
            score = jnp.where(live, score, -1e30)
            expo = jnp.exp(score - jnp.max(score, axis=0, keepdims=True))
            prob = expo * (1.0 / jnp.sum(expo, axis=0, keepdims=True))
            whole = jnp.broadcast_to(jnp.sum(prob, axis=0, keepdims=True), (8, half))
            shares.append(jnp.concatenate([prob * scale, whole], axis=0))
        wide = jnp.dot(
            widen, jnp.concatenate(shares, axis=1).astype(BF16), preferred_element_type=F32
        )
        for h in range(local_heads):
            weight = wide[:, h * half : (h + 1) * half] * field_ref[j]
            weight_ref[j, :, h * rows : (h + 1) * rows] = weight.T.astype(BF16)

    for get in get_values:
        get.wait()
    strip_heads = local_heads // halves
    of_column = lax.broadcasted_iota(jnp.int32, (rows, strip), 1) // head_size
    for a in range(halves):
        projected = jnp.dot(left[hi], value_all[a, hi], preferred_element_type=F32)
        for off in ring[::-1]:
            src = (hi + hi_size - off) % hi_size
            remote(
                value_all.at[a, src],
                value_all.at[a, src],
                send_sem.at[2],
                value_rs.at[a, off],
                here,
            ).wait_recv()
            projected += jnp.dot(left[src], value_all[a, src], preferred_element_type=F32)
        for far in range(lo_size - 1, -1, -1):
            j = flipped(lo, far)
            part = projected[:rows]
            for other in range(1, lo_size):
                part = jnp.where(j == other, projected[other * rows : (other + 1) * rows], part)
            spread = jnp.concatenate(
                [jnp.where(of_column == h, part, 0.0) for h in range(strip_heads)], axis=0
            ).astype(BF16)
            these = slice(a * strip_heads * rows, (a + 1) * strip_heads * rows)
            mixed = jnp.dot(weight_ref[j, :, these], spread, preferred_element_type=F32)
            mix_send[a, pl.ds(j * groups, groups)] = mixed.astype(BF16).reshape(
                groups, owned, strip
            )
            for near in range(groups - 1, -1, -1):
                bits = far * groups + near
                if bits:
                    to = flipped(mixer, bits)
                    there = {"dp": hi * lo_size + to // groups, "var": r * groups + to % groups}
                    remote(
                        mix_send.at[a, to],
                        mix_recv.at[a, mixer],
                        send_sem.at[5],
                        mix_rs.at[a, bits],
                        there,
                    ).start()

    get_out.wait()
    total = jnp.zeros((owned, width), F32)
    for a in range(halves):
        for near in range(groups):
            summed = None
            for far in range(lo_size):
                bits = far * groups + near
                src = flipped(mixer, bits)
                if bits:
                    remote(
                        mix_send.at[a, src],
                        mix_recv.at[a, src],
                        send_sem.at[5],
                        mix_rs.at[a, bits],
                        here,
                    ).wait_recv()
                    part = mix_recv[a, src].astype(F32)
                else:
                    part = mix_send[a, src].astype(F32)
                summed = part if summed is None else summed + part
            total += jnp.dot(
                summed.astype(BF16),
                wout[strip_of(flipped(g, near), a), :],
                preferred_element_type=F32,
            )
    result_ref[0] = total.astype(result_ref.dtype)

    all_ids.wait_send()
    all_pixels.wait_send()
    all_folds.wait_send()
    all_scales.wait_send()
    for a in range(halves):
        arrived(value_all.at[a], hi_size - 1, send_sem.at[2], value_rs.at[0, 0]).wait_send()
        arrived(mix_send.at[a], mixers - 1, send_sem.at[5], mix_rs.at[0, 0]).wait_send()


def on_device(
    n,
    nv,
    pixels,
    var_ids,
    counts,
    patch_weight,
    var_embed,
    norm_gain,
    norm_bias,
    key_weight,
    value_weight,
    query,
    out_weight,
):
    slots, taps, patches = pixels.shape[1:]
    width = out_weight.shape[0]
    heads, head_size = query.shape
    groups = min(nv, width // 128)
    lo_size = 2 if n % 2 == 0 else 1
    hi_size = n // lo_size
    team = lo_size * nv
    mixers = lo_size * groups
    columns = width // groups
    halves = 2 if columns % 256 == 0 else 1
    strip = columns // halves
    depth = value_weight.shape[0]
    padded = rounded_up(slots, 8)
    owned = patches // nv
    half = patches * groups // nv
    local_heads = heads // groups
    fold_rows = rounded_up(local_heads, 8)
    every = nv * slots
    rows = rounded_up(every * taps + every + 1, 16)
    hbm = pl.BlockSpec(memory_space=pltpu.HBM)
    vmem = pl.BlockSpec(memory_space=pltpu.VMEM)
    dims = (n, nv, groups, lo_size, slots, taps, patches, width, heads, head_size)
    dma = pltpu.SemaphoreType.DMA
    return pl.pallas_call(
        functools.partial(kernel, dims),
        out_shape=pltpu.VMEM((1, owned, width), BF16),
        in_specs=[hbm] * 11,
        out_specs=vmem,
        scratch_shapes=[
            pltpu.SMEM((team,) + var_ids.shape, jnp.int32),
            pltpu.SMEM(counts.shape, jnp.int32),
            pltpu.VMEM((team, slots, taps, patches), BF16),
            pltpu.VMEM(patch_weight.shape, BF16),
            pltpu.VMEM(var_embed.shape, BF16),
            pltpu.VMEM((1, width), F32),
            pltpu.VMEM((1, width), F32),
            pltpu.VMEM(query.shape, F32),
            pltpu.VMEM((depth, columns), BF16),
            pltpu.VMEM((halves, depth, strip), BF16),
            pltpu.VMEM((halves, hi_size, depth, strip), BF16),
            pltpu.VMEM((width, width), BF16),
            pltpu.VMEM((n, fold_rows, depth), F32),
            pltpu.VMEM((taps + 1, padded, width), F32),
            pltpu.VMEM((lo_size, rows, width), F32),
            pltpu.VMEM((hi_size, lo_size * rows, depth), BF16),
            pltpu.VMEM((lo_size, rows, half), F32),
            pltpu.VMEM((team, padded, patches), F32),
            pltpu.VMEM((lo_size, every, half), F32),
            pltpu.VMEM((lo_size, local_heads * every, half), F32),
            pltpu.VMEM((lo_size, half, local_heads * rows), BF16),
            pltpu.VMEM((halves, mixers, owned, strip), BF16),
            pltpu.VMEM((halves, mixers, owned, strip), BF16),
            dma((10 + 2 * halves,)),
            dma((6,)),
            dma((4,)),
            dma((halves, hi_size)),
            dma((halves, mixers)),
        ],
        compiler_params=pltpu.CompilerParams(collective_id=0, has_side_effects=True),
    )(
        pixels,
        var_ids,
        counts,
        patch_weight,
        var_embed,
        norm_gain.reshape(1, width),
        norm_bias.reshape(1, width),
        key_weight,
        value_weight,
        query,
        out_weight,
    )


def solution(mesh):
    placed = (
        P("dp", "var", None, None),
        P("dp", "var"),
        P("dp"),
        P(),
        P(),
        P(),
        P(),
        P("dp", None),
        P("dp", None),
        P(),
        P(),
    )
    return jax.shard_map(
        functools.partial(on_device, mesh.shape["dp"], mesh.shape["var"]),
        mesh=mesh,
        in_specs=placed,
        out_specs=P("dp", "var", None),
        check_vma=False,
    )
```

```python
import functools
import math

import jax
import jax.numpy as jnp
from jax import lax
from jax.experimental import pallas as pl
from jax.experimental.pallas import tpu as pltpu
from jax.sharding import PartitionSpec as P

F32 = jnp.float32
BF16 = jnp.bfloat16
MESH = pl.DeviceIdType.MESH
PIECES = 3


def rounded_up(value, unit):
    return -(-value // unit) * unit


class Bits:
    def __init__(self, index, size):
        self.index = index
        self.steps = {}
        bit = 1
        while bit < size:
            self.steps[bit] = bit - 2 * bit * lax.rem(lax.div(index, bit), 2)
            bit *= 2

    def flip(self, bits):
        index = self.index
        for bit, step in self.steps.items():
            if bits & bit:
                index = index + step
        return index


def pieces_of(value):
    parts = []
    for _ in range(PIECES):
        part = value.astype(BF16).astype(F32)
        parts.append(part)
        value = value - part
    return parts


def kernel(
    dims,
    pixels_hbm,
    ids_hbm,
    counts_hbm,
    table_hbm,
    embed_hbm,
    gain_hbm,
    bias_hbm,
    key_hbm,
    value_hbm,
    query_hbm,
    out_hbm,
    result_ref,
    ids_all,
    counts_ref,
    pix_all,
    table,
    embed,
    gain_ref,
    bias_ref,
    query_ref,
    key_block,
    value_send,
    value_all,
    wout,
    fold_all,
    own_rows,
    raw,
    left,
    field_ref,
    scale_all,
    scale_ref,
    score_ref,
    weight_ref,
    mix_send,
    mix_recv,
    local_sem,
    send_sem,
    once_sem,
    value_rs,
    mix_rs,
    hand,
):
    n, nv, groups, lo_size, slots, taps, patches, width, heads, head_size = dims
    hi_size = n // lo_size
    team = lo_size * nv
    mixers = lo_size * groups
    depth = key_block.shape[0]
    columns = key_block.shape[1]
    halves = value_all.shape[0]
    strip = columns // halves
    crossed = groups % 2 == 0
    local_heads = heads // groups
    fold_rows = fold_all.shape[1]
    half = patches * groups // nv
    owned = patches // nv
    padded = own_rows.shape[1]
    every = nv * slots
    tap_rows = every * taps
    rows = raw.shape[1]
    tail = rows - tap_rows - every

    b = lax.axis_index("dp")
    v = lax.axis_index("var")
    hi, lo = lax.div(b, lo_size), lax.rem(b, lo_size)
    r, g = lax.div(v, groups), lax.rem(v, groups)
    me = lo * nv + v
    mixer = lo * groups + g
    my_lo, my_v = Bits(lo, lo_size), Bits(v, nv)
    first_b = b - lo

    def mate(bits):
        return {"dp": first_b + my_lo.flip(bits // nv), "var": my_v.flip(bits % nv)}

    def partner_of(bits):
        far, near = bits // groups, bits % groups
        there = my_v.flip(near)
        return my_lo.flip(far) * groups + there - r * groups, {
            "dp": first_b + my_lo.flip(far),
            "var": there,
        }

    def other_than(index, k):
        return k + jnp.where(index <= k, 1, 0)

    rings = [other_than(hi, k) for k in range(hi_size - 1)]

    def remote(src, dst, ss, rs, where):
        return pltpu.make_async_remote_copy(
            src_ref=src, dst_ref=dst, send_sem=ss, recv_sem=rs, device_id=where, device_id_type=MESH
        )

    here = {"dp": b, "var": v}
    to_core = my_v.flip(1) if crossed else v
    to_group = to_core - r * groups

    mine = pl.ds(pl.multiple_of(g * columns, columns), columns)

    def strip_of(group, a):
        return pl.ds(pl.multiple_of(group * columns + a * strip, strip), strip)

    copies = [
        (query_hbm, query_ref),
        (key_hbm.at[:, mine], key_block),
        (ids_hbm, ids_all.at[me]),
        (pixels_hbm.at[0], pix_all.at[me]),
        (table_hbm, table),
        (embed_hbm, embed),
        (gain_hbm, gain_ref),
        (bias_hbm, bias_ref),
        (counts_hbm, counts_ref),
        (out_hbm, wout),
    ]
    copies += [(value_hbm.at[:, strip_of(g, a)], value_all.at[a, hi]) for a in range(halves)]
    copies[2:2] = [
        (value_hbm.at[:, strip_of(to_group, a)], value_send.at[a]) for a in range(halves)
    ]
    gets = [pltpu.make_async_copy(s, d, local_sem.at[i]) for i, (s, d) in enumerate(copies)]
    for get in gets:
        get.start()

    barrier = pltpu.get_barrier_semaphore()

    def greet(where):
        pl.semaphore_signal(barrier, inc=1, device_id=where, device_id_type=MESH)

    core = lax.rem(v, 2)
    partner = {"var": my_v.flip(1)}
    if crossed:
        for k, to in enumerate(rings):
            ear = 1 if k == 0 else jnp.where(hi == 0, 1, 0)
            for other in range(lo_size):
                greet({"dp": to * lo_size + other, "var": v - core + ear})

        @pl.when(core == 0)
        def _():
            greet(partner)
            for bits in range(2, team, 2):
                greet(mate(bits))

        @pl.when(core == 1)
        def _():
            for bits in range(1, team, 2):
                greet(mate(bits))
    else:
        for to in rings:
            for other in range(lo_size):
                greet({"dp": to * lo_size + other})
        for bits in range(1, team):
            greet(mate(bits))

    get_query, get_key = gets[:2]
    get_strips = gets[2 : 2 + halves]
    get_values = gets[-halves:]
    (
        get_ids,
        get_pixels,
        get_table,
        get_embed,
        get_gain,
        get_bias,
        get_counts,
        get_out,
    ) = gets[2 + halves : -halves]

    get_query.wait()
    own_query = query_ref[:local_heads]
    for i in range(1, groups):
        own_query = jnp.where(
            g == i, query_ref[i * local_heads : (i + 1) * local_heads], own_query
        )
    own_query = own_query * (1.0 / math.sqrt(head_size))
    if fold_rows > local_heads:
        blank = jnp.zeros((fold_rows - local_heads, head_size), F32)
        own_query = jnp.concatenate([own_query, blank], axis=0)
    own_head = (
        lax.broadcasted_iota(jnp.int32, (fold_rows, columns), 1) // head_size
        == lax.broadcasted_iota(jnp.int32, (fold_rows, columns), 0)
    )
    diagonal = jnp.where(own_head, jnp.concatenate([own_query] * local_heads, axis=1), 0.0)
    diagonal = jnp.concatenate(pieces_of(diagonal), axis=0).astype(BF16)
    get_key.wait()
    found = lax.dot_general(
        diagonal, key_block[...], (((1,), (1,)), ((), ())), preferred_element_type=F32
    )
    fold = found[:fold_rows]
    for i in range(1, PIECES):
        fold = fold + found[i * fold_rows : (i + 1) * fold_rows]
    fold_all[b] = fold

    for get in get_strips:
        get.wait()
    get_ids.wait()
    get_pixels.wait()

    def send_fold(there):
        remote(fold_all.at[b], fold_all.at[b], send_sem.at[3], once_sem.at[2], there).start()

    def send_rows(some):
        for to in some:
            for other in range(lo_size):
                send_fold({"dp": to * lo_size + other})
        for a in range(halves):
            for to in some:
                there = {"dp": to * lo_size + lo, "var": to_core}
                remote(
                    value_send.at[a],
                    value_all.at[a, hi],
                    send_sem.at[2],
                    value_rs.at[a, hi],
                    there,
                ).start()

    def send_team():
        for bits in range(1, team):
            where = mate(bits)
            remote(ids_all.at[me], ids_all.at[me], send_sem.at[0], once_sem.at[0], where).start()
            remote(pix_all.at[me], pix_all.at[me], send_sem.at[1], once_sem.at[1], where).start()
        for far in range(1, lo_size):
            send_fold({"dp": first_b + my_lo.flip(far)})

    def tell_partner():
        pl.semaphore_signal(hand, inc=1, device_id=partner, device_id_type=MESH)

    if crossed:
        early, even = hi == 0, core == 0

        @pl.when(early & even)
        def _():
            pl.semaphore_wait(barrier, team - 1)
            tell_partner()
            send_team()
            pl.semaphore_wait(hand, 1)
            send_rows(rings)

        @pl.when(early & ~even)
        def _():
            pl.semaphore_wait(hand, 1)
            send_team()
            pl.semaphore_wait(barrier, 2 * (n - lo_size) + 1)
            tell_partner()
            send_rows(rings)

        @pl.when(~early & even)
        def _():
            pl.semaphore_wait(hand, 1)
            send_rows(rings[:1])
            pl.semaphore_wait(barrier, team - 1 + 2 * (n - 2 * lo_size))
            tell_partner()
            send_rows(rings[1:])
            send_team()

        @pl.when(~early & ~even)
        def _():
            pl.semaphore_wait(barrier, 2 * lo_size + 1)
            tell_partner()
            send_rows(rings[:1])
            pl.semaphore_wait(hand, 1)
            send_rows(rings[1:])
            send_team()

    else:
        pl.semaphore_wait(barrier, n - lo_size + team - 1)
        send_rows(rings)
        send_team()

    get_table.wait()
    get_embed.wait()
    own_rows[...] = jnp.zeros_like(own_rows)
    ids_at = lax.broadcasted_iota(jnp.int32, (padded, embed.shape[0]), 0)
    wanted = jnp.full((padded, embed.shape[0]), -1, jnp.int32)
    for s in range(slots):
        chosen = ids_all[me, 0, s]
        found = table[chosen].astype(F32)
        for k in range(taps):
            own_rows[k, s : s + 1, :] = found[k : k + 1, :]
        wanted = jnp.where(ids_at == s, chosen, wanted)
    hot = (wanted == lax.broadcasted_iota(jnp.int32, wanted.shape, 1)).astype(BF16)
    own_rows[taps] = jnp.dot(hot, embed[...], preferred_element_type=F32)
    centred = []
    for k in range(taps + 1):
        row = own_rows[k]
        centred.append(row - jnp.mean(row, axis=-1, keepdims=True))
    pix = pix_all[me].astype(F32)
    fill = jnp.zeros((padded - slots, patches), F32)
    field = []
    for k in range(taps):
        own = [pix[s, k : k + 1, :] for s in range(slots)]
        field.append(jnp.concatenate(own + ([fill] if padded > slots else []), axis=0))
    field.append(jnp.ones((padded, patches), F32))
    variance = jnp.zeros((padded, patches), F32)
    for k in range(taps + 1):
        for m in range(k, taps + 1):
            gram = jnp.mean(centred[k] * centred[m], axis=-1, keepdims=True)
            variance += (1.0 if m == k else 2.0) * gram * (field[k] * field[m])
    scale = lax.rsqrt(jnp.maximum(variance, 0.0) + 1e-05)
    get_counts.wait()
    place = lax.broadcasted_iota(jnp.int32, (padded, patches), 0)
    live = (place < slots) & (v * slots + place < counts_ref[0])
    scale_all[me] = jnp.where(live, scale, -1.0)
    for bits in range(team - 1, 0, -1):
        remote(
            scale_all.at[me], scale_all.at[me], send_sem.at[4], once_sem.at[3], mate(bits)
        ).start()

    def arrived(ref, count, ss, rs):
        block = ref.at[pl.ds(0, count)]
        return remote(block, block, ss, rs, here)

    all_ids = arrived(ids_all, team - 1, send_sem.at[0], once_sem.at[0])
    all_ids.wait_recv()
    get_gain.wait()
    get_bias.wait()
    gain = gain_ref[...]
    slot_at = lax.broadcasted_iota(jnp.int32, (every, embed.shape[0]), 0)
    for j in range(lo_size):
        wanted = jnp.full((every, embed.shape[0]), -1, jnp.int32)
        for s in range(every):
            chosen = ids_all[j * nv + s // slots, 0, s % slots]
            raw[j, s * taps : (s + 1) * taps, :] = table[chosen].astype(F32)
            wanted = jnp.where(slot_at == s, chosen, wanted)
        hot = (wanted == lax.broadcasted_iota(jnp.int32, wanted.shape, 1)).astype(BF16)
        raw[j, tap_rows : tap_rows + every, :] = jnp.dot(
            hot, embed[...], preferred_element_type=F32
        )
        raw[j, tap_rows + every :, :] = jnp.zeros((tail, width), F32)
        row = raw[j, : tap_rows + every, :]
        row = (row - jnp.mean(row, axis=-1, keepdims=True)) * gain
        last = lax.broadcasted_iota(jnp.int32, (tail, width), 0)
        last = jnp.where(last == 0, bias_ref[...], 0.0)
        basis = jnp.concatenate([row, last], axis=0)
        for h in range(hi_size):
            at = h * lo_size * depth
            part = basis[:, at : at + depth]
            for other in range(1, lo_size):
                at += depth
                part = jnp.where(lo == other, basis[:, at : at + depth], part)
            left[h, j * rows : (j + 1) * rows, :] = part.astype(BF16)

    all_folds = arrived(fold_all, n - 1, send_sem.at[3], once_sem.at[2])
    all_folds.wait_recv()
    folded = jnp.concatenate([fold_all[i] for i in range(n)], axis=1)
    bias_score = jnp.sum(folded * bias_ref[...], axis=-1, keepdims=True)
    folded = folded * gain
    fold_sum = jnp.sum(folded, axis=-1, keepdims=True)
    keys = jnp.concatenate(pieces_of(folded) + [jnp.ones((8, width), F32)], axis=0).astype(BF16)

    which = lax.broadcasted_iota(jnp.int32, (every, rows), 0)
    what = lax.broadcasted_iota(jnp.int32, (every, rows), 1)
    of_slot = jnp.where(what < tap_rows, what // taps, what - tap_rows) == which
    to_row = lax.broadcasted_iota(jnp.int32, (rows, every + 8), 0)
    of_row = jnp.where(to_row < tap_rows, to_row // taps, to_row - tap_rows)
    widen = (of_row == lax.broadcasted_iota(jnp.int32, (rows, every + 8), 1)).astype(BF16)

    blocks = []
    for j in range(lo_size):
        found = lax.dot_general(
            keys, raw[j].astype(BF16), (((1,), (1,)), ((), ())), preferred_element_type=F32
        )
        score_of = found[:fold_rows]
        for i in range(1, PIECES):
            score_of = score_of + found[i * fold_rows : (i + 1) * fold_rows]
        row_sum = found[PIECES * fold_rows : PIECES * fold_rows + 1]
        score_of = score_of - (row_sum * (1.0 / width)) * fold_sum
        parts = [
            jnp.where(of_slot, part[h : h + 1, :], 0.0)
            for part in pieces_of(score_of)
            for h in range(local_heads)
        ]
        blocks.append(jnp.concatenate(parts, axis=0).astype(BF16))

    all_pixels = arrived(pix_all, team - 1, send_sem.at[1], once_sem.at[1])
    all_pixels.wait_recv()
    window = pl.ds(pl.multiple_of(r * half, half), half)
    for j in range(lo_size):
        for s in range(every):
            field_ref[j, s * taps : (s + 1) * taps, :] = pix_all[
                j * nv + s // slots, s % slots, :, window
            ].astype(F32)
        field_ref[j, tap_rows:, :] = jnp.ones((rows - tap_rows, half), F32)
        found = jnp.dot(blocks[j], field_ref[j].astype(BF16), preferred_element_type=F32)
        every_head = local_heads * every
        score = found[:every_head]
        for i in range(1, PIECES):
            score = score + found[i * every_head : (i + 1) * every_head]
        score_ref[j] = score

    all_scales = arrived(scale_all, team - 1, send_sem.at[4], once_sem.at[3])
    all_scales.wait_recv()
    for j in range(lo_size):
        for i in range(nv):
            scale_ref[j, i * slots : (i + 1) * slots, :] = scale_all[j * nv + i, :slots, window]
        scale = scale_ref[j]
        live = scale > 0.0
        shares = []
        for h in range(local_heads):
            score = score_ref[j, h * every : (h + 1) * every, :]
            score = score * scale + bias_score[h : h + 1, :]
            score = jnp.where(live, score, -1e30)
            expo = jnp.exp(score - jnp.max(score, axis=0, keepdims=True))
            prob = expo * (1.0 / jnp.sum(expo, axis=0, keepdims=True))
            whole = jnp.broadcast_to(jnp.sum(prob, axis=0, keepdims=True), (8, half))
            shares.append(jnp.concatenate([prob * scale, whole], axis=0))
        wide = jnp.dot(
            widen, jnp.concatenate(shares, axis=1).astype(BF16), preferred_element_type=F32
        )
        for h in range(local_heads):
            weight = wide[:, h * half : (h + 1) * half] * field_ref[j]
            weight_ref[j, :, h * rows : (h + 1) * rows] = weight.T.astype(BF16)

    for get in get_values:
        get.wait()
    strip_heads = local_heads // halves
    of_column = lax.broadcasted_iota(jnp.int32, (rows, strip), 1) // head_size
    for a in range(halves):
        projected = jnp.dot(left[hi], value_all[a, hi], preferred_element_type=F32)
        for src in rings:
            remote(
                value_all.at[a, src],
                value_all.at[a, src],
                send_sem.at[2],
                value_rs.at[a, src],
                here,
            ).wait_recv()
            projected += jnp.dot(left[src], value_all[a, src], preferred_element_type=F32)
        sent = 0
        for j in range(lo_size):
            part = projected[j * rows : (j + 1) * rows]
            spread = jnp.concatenate(
                [jnp.where(of_column == h, part, 0.0) for h in range(strip_heads)], axis=0
            ).astype(BF16)
            these = slice(a * strip_heads * rows, (a + 1) * strip_heads * rows)
            mixed = jnp.dot(weight_ref[j, :, these], spread, preferred_element_type=F32)
            mix_send[a, j * groups : (j + 1) * groups] = mixed.astype(BF16).reshape(
                groups, owned, strip
            )
            ready = (j + 1) * groups - 1
            for k in range(sent, ready):
                to = other_than(mixer, k)
                to_lo = lax.div(to, groups)
                there = {"dp": first_b + to_lo, "var": (r - to_lo) * groups + to}
                remote(
                    mix_send.at[a, to],
                    mix_recv.at[a, mixer],
                    send_sem.at[5],
                    mix_rs.at[a, mixer],
                    there,
                ).start()
            sent = ready

    get_out.wait()
    total = jnp.zeros((owned, width), F32)
    for a in range(halves):
        for near in range(groups):
            summed = None
            for far in range(lo_size):
                bits = far * groups + near
                src, _ = partner_of(bits)
                if bits:
                    remote(
                        mix_send.at[a, src],
                        mix_recv.at[a, src],
                        send_sem.at[5],
                        mix_rs.at[a, src],
                        here,
                    ).wait_recv()
                    part = mix_recv[a, src].astype(F32)
                else:
                    part = mix_send[a, src].astype(F32)
                summed = part if summed is None else summed + part
            total += jnp.dot(
                summed.astype(BF16),
                wout[strip_of(my_v.flip(near) - r * groups, a), :],
                preferred_element_type=F32,
            )
    result_ref[0] = total.astype(result_ref.dtype)

    all_ids.wait_send()
    all_pixels.wait_send()
    all_folds.wait_send()
    all_scales.wait_send()
    for a in range(halves):
        arrived(value_all.at[a], hi_size - 1, send_sem.at[2], value_rs.at[0, 0]).wait_send()
        arrived(mix_send.at[a], mixers - 1, send_sem.at[5], mix_rs.at[0, 0]).wait_send()


def on_device(
    n,
    nv,
    pixels,
    var_ids,
    counts,
    patch_weight,
    var_embed,
    norm_gain,
    norm_bias,
    key_weight,
    value_weight,
    query,
    out_weight,
):
    slots, taps, patches = pixels.shape[1:]
    width = out_weight.shape[0]
    heads, head_size = query.shape
    groups = min(nv, width // 128)
    lo_size = 2 if n % 2 == 0 else 1
    hi_size = n // lo_size
    team = lo_size * nv
    mixers = lo_size * groups
    columns = width // groups
    halves = 2 if columns % 256 == 0 else 1
    strip = columns // halves
    depth = value_weight.shape[0]
    padded = rounded_up(slots, 8)
    owned = patches // nv
    half = patches * groups // nv
    local_heads = heads // groups
    fold_rows = rounded_up(local_heads, 8)
    every = nv * slots
    rows = rounded_up(every * taps + every + 1, 16)
    hbm = pl.BlockSpec(memory_space=pltpu.HBM)
    vmem = pl.BlockSpec(memory_space=pltpu.VMEM)
    dims = (n, nv, groups, lo_size, slots, taps, patches, width, heads, head_size)
    dma = pltpu.SemaphoreType.DMA
    return pl.pallas_call(
        functools.partial(kernel, dims),
        out_shape=pltpu.VMEM((1, owned, width), BF16),
        in_specs=[hbm] * 11,
        out_specs=vmem,
        scratch_shapes=[
            pltpu.SMEM((team,) + var_ids.shape, jnp.int32),
            pltpu.SMEM(counts.shape, jnp.int32),
            pltpu.VMEM((team, slots, taps, patches), BF16),
            pltpu.VMEM(patch_weight.shape, BF16),
            pltpu.VMEM(var_embed.shape, BF16),
            pltpu.VMEM((1, width), F32),
            pltpu.VMEM((1, width), F32),
            pltpu.VMEM(query.shape, F32),
            pltpu.VMEM((depth, columns), BF16),
            pltpu.VMEM((halves, depth, strip), BF16),
            pltpu.VMEM((halves, hi_size, depth, strip), BF16),
            pltpu.VMEM((width, width), BF16),
            pltpu.VMEM((n, fold_rows, depth), F32),
            pltpu.VMEM((taps + 1, padded, width), F32),
            pltpu.VMEM((lo_size, rows, width), F32),
            pltpu.VMEM((hi_size, lo_size * rows, depth), BF16),
            pltpu.VMEM((lo_size, rows, half), F32),
            pltpu.VMEM((team, padded, patches), F32),
            pltpu.VMEM((lo_size, every, half), F32),
            pltpu.VMEM((lo_size, local_heads * every, half), F32),
            pltpu.VMEM((lo_size, half, local_heads * rows), BF16),
            pltpu.VMEM((halves, mixers, owned, strip), BF16),
            pltpu.VMEM((halves, mixers, owned, strip), BF16),
            dma((10 + 2 * halves,)),
            dma((6,)),
            dma((4,)),
            dma((halves, hi_size)),
            dma((halves, mixers)),
            pltpu.SemaphoreType.REGULAR,
        ],
        compiler_params=pltpu.CompilerParams(collective_id=0, has_side_effects=True),
    )(
        pixels,
        var_ids,
        counts,
        patch_weight,
        var_embed,
        norm_gain.reshape(1, width),
        norm_bias.reshape(1, width),
        key_weight,
        value_weight,
        query,
        out_weight,
    )


def solution(mesh):
    placed = (
        P("dp", "var", None, None),
        P("dp", "var"),
        P("dp"),
        P(),
        P(),
        P(),
        P(),
        P("dp", None),
        P("dp", None),
        P(),
        P(),
    )
    return jax.shard_map(
        functools.partial(on_device, mesh.shape["dp"], mesh.shape["var"]),
        mesh=mesh,
        in_specs=placed,
        out_specs=P("dp", "var", None),
        check_vma=False,
    )
```

```python
import functools
import math

import jax
import jax.numpy as jnp
from jax import lax
from jax.experimental import pallas as pl
from jax.experimental.pallas import tpu as pltpu
from jax.sharding import PartitionSpec as P

F32 = jnp.float32
BF16 = jnp.bfloat16
MESH = pl.DeviceIdType.MESH
PIECES = 3


def rounded_up(value, unit):
    return -(-value // unit) * unit


class Bits:
    def __init__(self, index, size):
        self.index = index
        self.steps = {}
        bit = 1
        while bit < size:
            self.steps[bit] = bit - 2 * bit * lax.rem(lax.div(index, bit), 2)
            bit *= 2

    def flip(self, bits):
        index = self.index
        for bit, step in self.steps.items():
            if bits & bit:
                index = index + step
        return index


def pieces_of(value):
    parts = []
    for _ in range(PIECES):
        part = value.astype(BF16).astype(F32)
        parts.append(part)
        value = value - part
    return parts


def kernel(
    dims,
    pixels_hbm,
    ids_hbm,
    counts_hbm,
    table_hbm,
    embed_hbm,
    gain_hbm,
    bias_hbm,
    key_hbm,
    value_hbm,
    query_hbm,
    out_hbm,
    result_ref,
    ids_all,
    counts_ref,
    pix_all,
    table,
    embed,
    gain_ref,
    bias_ref,
    query_ref,
    key_block,
    value_send,
    value_all,
    wout,
    fold_all,
    own_rows,
    raw,
    left,
    field_ref,
    scale_all,
    scale_ref,
    score_ref,
    weight_ref,
    mix_send,
    mix_recv,
    local_sem,
    send_sem,
    once_sem,
    value_rs,
    mix_rs,
    hand,
):
    n, nv, groups, lo_size, slots, taps, patches, width, heads, head_size = dims
    hi_size = n // lo_size
    team = lo_size * nv
    mixers = lo_size * groups
    depth = key_block.shape[0]
    columns = key_block.shape[1]
    halves = value_all.shape[0]
    strip = columns // halves
    crossed = groups % 2 == 0
    local_heads = heads // groups
    fold_rows = fold_all.shape[1]
    half = patches * groups // nv
    owned = patches // nv
    padded = own_rows.shape[1]
    every = nv * slots
    tap_rows = every * taps
    rows = raw.shape[1]
    tail = rows - tap_rows - every

    b = lax.axis_index("dp")
    v = lax.axis_index("var")
    hi, lo = lax.div(b, lo_size), lax.rem(b, lo_size)
    r, g = lax.div(v, groups), lax.rem(v, groups)
    me = lo * nv + v
    mixer = lo * groups + g
    my_lo, my_v = Bits(lo, lo_size), Bits(v, nv)
    first_b = b - lo

    def mate(bits):
        return {"dp": first_b + my_lo.flip(bits // nv), "var": my_v.flip(bits % nv)}

    def partner_of(bits):
        far, near = bits // groups, bits % groups
        there = my_v.flip(near)
        return my_lo.flip(far) * groups + there - r * groups, {
            "dp": first_b + my_lo.flip(far),
            "var": there,
        }

    def other_than(index, k):
        return k + jnp.where(index <= k, 1, 0)

    rings = [other_than(hi, k) for k in range(hi_size - 1)]

    def remote(src, dst, ss, rs, where):
        return pltpu.make_async_remote_copy(
            src_ref=src, dst_ref=dst, send_sem=ss, recv_sem=rs, device_id=where, device_id_type=MESH
        )

    here = {"dp": b, "var": v}
    to_core = my_v.flip(1) if crossed else v
    to_group = to_core - r * groups

    mine = pl.ds(pl.multiple_of(g * columns, columns), columns)

    def strip_of(group, a):
        return pl.ds(pl.multiple_of(group * columns + a * strip, strip), strip)

    copies = [
        (query_hbm, query_ref),
        (key_hbm.at[:, mine], key_block),
        (ids_hbm, ids_all.at[me]),
        (pixels_hbm.at[0], pix_all.at[me]),
        (table_hbm, table),
        (embed_hbm, embed),
        (gain_hbm, gain_ref),
        (bias_hbm, bias_ref),
        (counts_hbm, counts_ref),
        (out_hbm, wout),
    ]
    copies += [(value_hbm.at[:, strip_of(g, a)], value_all.at[a, hi]) for a in range(halves)]
    copies[2:2] = [
        (value_hbm.at[:, strip_of(to_group, a)], value_send.at[a]) for a in range(halves)
    ]
    gets = [pltpu.make_async_copy(s, d, local_sem.at[i]) for i, (s, d) in enumerate(copies)]
    for get in gets:
        get.start()

    barrier = pltpu.get_barrier_semaphore()

    def greet(where):
        pl.semaphore_signal(barrier, inc=1, device_id=where, device_id_type=MESH)

    core = lax.rem(v, 2)
    partner = {"var": my_v.flip(1)}
    if crossed:
        for k, to in enumerate(rings):
            ear = 1 if k == 0 else jnp.where(hi == 0, 1, 0)
            for other in range(lo_size):
                greet({"dp": to * lo_size + other, "var": v - core + ear})

        @pl.when(core == 0)
        def _():
            greet(partner)
            for bits in range(2, team, 2):
                greet(mate(bits))

        @pl.when(core == 1)
        def _():
            for bits in range(1, team, 2):
                greet(mate(bits))
    else:
        for to in rings:
            for other in range(lo_size):
                greet({"dp": to * lo_size + other})
        for bits in range(1, team):
            greet(mate(bits))

    get_query, get_key = gets[:2]
    get_strips = gets[2 : 2 + halves]
    get_values = gets[-halves:]
    (
        get_ids,
        get_pixels,
        get_table,
        get_embed,
        get_gain,
        get_bias,
        get_counts,
        get_out,
    ) = gets[2 + halves : -halves]

    get_query.wait()
    own_query = query_ref[:local_heads]
    for i in range(1, groups):
        own_query = jnp.where(
            g == i, query_ref[i * local_heads : (i + 1) * local_heads], own_query
        )
    own_query = own_query * (1.0 / math.sqrt(head_size))
    if fold_rows > local_heads:
        blank = jnp.zeros((fold_rows - local_heads, head_size), F32)
        own_query = jnp.concatenate([own_query, blank], axis=0)
    own_head = (
        lax.broadcasted_iota(jnp.int32, (fold_rows, columns), 1) // head_size
        == lax.broadcasted_iota(jnp.int32, (fold_rows, columns), 0)
    )
    diagonal = jnp.where(own_head, jnp.concatenate([own_query] * local_heads, axis=1), 0.0)
    diagonal = jnp.concatenate(pieces_of(diagonal), axis=0).astype(BF16)
    get_key.wait()
    found = lax.dot_general(
        diagonal, key_block[...], (((1,), (1,)), ((), ())), preferred_element_type=F32
    )
    fold = found[:fold_rows]
    for i in range(1, PIECES):
        fold = fold + found[i * fold_rows : (i + 1) * fold_rows]
    fold_all[b] = fold

    for get in get_strips:
        get.wait()
    get_ids.wait()
    get_pixels.wait()

    def send_fold(there):
        remote(fold_all.at[b], fold_all.at[b], send_sem.at[3], once_sem.at[2], there).start()

    def send_rows(some):
        for to in some:
            for other in range(lo_size):
                send_fold({"dp": to * lo_size + other})
        for a in range(halves):
            for to in some:
                there = {"dp": to * lo_size + lo, "var": to_core}
                remote(
                    value_send.at[a],
                    value_all.at[a, hi],
                    send_sem.at[2],
                    value_rs.at[a, hi],
                    there,
                ).start()

    def send_team():
        for bits in range(1, team):
            where = mate(bits)
            remote(ids_all.at[me], ids_all.at[me], send_sem.at[0], once_sem.at[0], where).start()
            remote(pix_all.at[me], pix_all.at[me], send_sem.at[1], once_sem.at[1], where).start()
        for far in range(1, lo_size):
            send_fold({"dp": first_b + my_lo.flip(far)})

    def tell_partner():
        pl.semaphore_signal(hand, inc=1, device_id=partner, device_id_type=MESH)

    if crossed:
        early, even = hi == 0, core == 0

        @pl.when(early & even)
        def _():
            pl.semaphore_wait(barrier, team - 1)
            tell_partner()
            send_team()
            pl.semaphore_wait(hand, 1)
            send_rows(rings)

        @pl.when(early & ~even)
        def _():
            pl.semaphore_wait(hand, 1)
            send_team()
            pl.semaphore_wait(barrier, 2 * (n - lo_size) + 1)
            tell_partner()
            send_rows(rings)

        @pl.when(~early & even)
        def _():
            pl.semaphore_wait(hand, 1)
            send_rows(rings[:1])
            pl.semaphore_wait(barrier, team - 1 + 2 * (n - 2 * lo_size))
            tell_partner()
            send_rows(rings[1:])
            send_team()

        @pl.when(~early & ~even)
        def _():
            pl.semaphore_wait(barrier, 2 * lo_size + 1)
            tell_partner()
            send_rows(rings[:1])
            pl.semaphore_wait(hand, 1)
            send_rows(rings[1:])
            send_team()

    else:
        pl.semaphore_wait(barrier, n - lo_size + team - 1)
        send_rows(rings)
        send_team()

    get_table.wait()
    get_embed.wait()
    own_rows[...] = jnp.zeros_like(own_rows)
    ids_at = lax.broadcasted_iota(jnp.int32, (padded, embed.shape[0]), 0)
    wanted = jnp.full((padded, embed.shape[0]), -1, jnp.int32)
    for s in range(slots):
        chosen = ids_all[me, 0, s]
        found = table[chosen].astype(F32)
        for k in range(taps):
            own_rows[k, s : s + 1, :] = found[k : k + 1, :]
        wanted = jnp.where(ids_at == s, chosen, wanted)
    hot = (wanted == lax.broadcasted_iota(jnp.int32, wanted.shape, 1)).astype(BF16)
    own_rows[taps] = jnp.dot(hot, embed[...], preferred_element_type=F32)
    centred = []
    for k in range(taps + 1):
        row = own_rows[k]
        centred.append(row - jnp.mean(row, axis=-1, keepdims=True))
    pix = pix_all[me].astype(F32)
    fill = jnp.zeros((padded - slots, patches), F32)
    field = []
    for k in range(taps):
        own = [pix[s, k : k + 1, :] for s in range(slots)]
        field.append(jnp.concatenate(own + ([fill] if padded > slots else []), axis=0))
    field.append(jnp.ones((padded, patches), F32))
    variance = jnp.zeros((padded, patches), F32)
    for k in range(taps + 1):
        for m in range(k, taps + 1):
            gram = jnp.mean(centred[k] * centred[m], axis=-1, keepdims=True)
            variance += (1.0 if m == k else 2.0) * gram * (field[k] * field[m])
    scale = lax.rsqrt(jnp.maximum(variance, 0.0) + 1e-05)
    get_counts.wait()
    place = lax.broadcasted_iota(jnp.int32, (padded, patches), 0)
    live = (place < slots) & (v * slots + place < counts_ref[0])
    scale_all[me] = jnp.where(live, scale, -1.0)
    for bits in range(team - 1, 0, -1):
        remote(
            scale_all.at[me], scale_all.at[me], send_sem.at[4], once_sem.at[3], mate(bits)
        ).start()

    def arrived(ref, count, ss, rs):
        block = ref.at[pl.ds(0, count)]
        return remote(block, block, ss, rs, here)

    all_ids = arrived(ids_all, team - 1, send_sem.at[0], once_sem.at[0])
    all_ids.wait_recv()
    get_gain.wait()
    get_bias.wait()
    gain = gain_ref[...]
    slot_at = lax.broadcasted_iota(jnp.int32, (every, embed.shape[0]), 0)
    for j in range(lo_size):
        wanted = jnp.full((every, embed.shape[0]), -1, jnp.int32)
        for s in range(every):
            chosen = ids_all[j * nv + s // slots, 0, s % slots]
            raw[j, s * taps : (s + 1) * taps, :] = table[chosen].astype(F32)
            wanted = jnp.where(slot_at == s, chosen, wanted)
        hot = (wanted == lax.broadcasted_iota(jnp.int32, wanted.shape, 1)).astype(BF16)
        raw[j, tap_rows : tap_rows + every, :] = jnp.dot(
            hot, embed[...], preferred_element_type=F32
        )
        raw[j, tap_rows + every :, :] = jnp.zeros((tail, width), F32)
        row = raw[j, : tap_rows + every, :]
        row = (row - jnp.mean(row, axis=-1, keepdims=True)) * gain
        last = lax.broadcasted_iota(jnp.int32, (tail, width), 0)
        last = jnp.where(last == 0, bias_ref[...], 0.0)
        basis = jnp.concatenate([row, last], axis=0)
        parts = []
        for h in range(hi_size):
            at = h * lo_size * depth
            part = basis[:, at : at + depth]
            for other in range(1, lo_size):
                at += depth
                part = jnp.where(lo == other, basis[:, at : at + depth], part)
            parts.append(part)
        left[j * rows : (j + 1) * rows, :] = jnp.concatenate(parts, axis=1).astype(BF16)

    all_folds = arrived(fold_all, n - 1, send_sem.at[3], once_sem.at[2])
    all_folds.wait_recv()
    folded = jnp.concatenate([fold_all[i] for i in range(n)], axis=1)
    bias_score = jnp.sum(folded * bias_ref[...], axis=-1, keepdims=True)
    folded = folded * gain
    fold_sum = jnp.sum(folded, axis=-1, keepdims=True)
    keys = jnp.concatenate(pieces_of(folded) + [jnp.ones((8, width), F32)], axis=0).astype(BF16)

    which = lax.broadcasted_iota(jnp.int32, (every, rows), 0)
    what = lax.broadcasted_iota(jnp.int32, (every, rows), 1)
    of_slot = jnp.where(what < tap_rows, what // taps, what - tap_rows) == which
    to_row = lax.broadcasted_iota(jnp.int32, (rows, every + 8), 0)
    of_row = jnp.where(to_row < tap_rows, to_row // taps, to_row - tap_rows)
    widen = (of_row == lax.broadcasted_iota(jnp.int32, (rows, every + 8), 1)).astype(BF16)

    blocks = []
    for j in range(lo_size):
        found = lax.dot_general(
            keys, raw[j].astype(BF16), (((1,), (1,)), ((), ())), preferred_element_type=F32
        )
        score_of = found[:fold_rows]
        for i in range(1, PIECES):
            score_of = score_of + found[i * fold_rows : (i + 1) * fold_rows]
        row_sum = found[PIECES * fold_rows : PIECES * fold_rows + 1]
        score_of = score_of - (row_sum * (1.0 / width)) * fold_sum
        parts = [
            jnp.where(of_slot, part[h : h + 1, :], 0.0)
            for part in pieces_of(score_of)
            for h in range(local_heads)
        ]
        blocks.append(jnp.concatenate(parts, axis=0).astype(BF16))

    all_pixels = arrived(pix_all, team - 1, send_sem.at[1], once_sem.at[1])
    all_pixels.wait_recv()
    window = pl.ds(pl.multiple_of(r * half, half), half)
    for j in range(lo_size):
        for s in range(every):
            field_ref[j, s * taps : (s + 1) * taps, :] = pix_all[
                j * nv + s // slots, s % slots, :, window
            ].astype(F32)
        field_ref[j, tap_rows:, :] = jnp.ones((rows - tap_rows, half), F32)
        found = jnp.dot(blocks[j], field_ref[j].astype(BF16), preferred_element_type=F32)
        every_head = local_heads * every
        score = found[:every_head]
        for i in range(1, PIECES):
            score = score + found[i * every_head : (i + 1) * every_head]
        score_ref[j] = score

    all_scales = arrived(scale_all, team - 1, send_sem.at[4], once_sem.at[3])
    all_scales.wait_recv()
    for j in range(lo_size):
        for i in range(nv):
            scale_ref[j, i * slots : (i + 1) * slots, :] = scale_all[j * nv + i, :slots, window]
        scale = scale_ref[j]
        live = scale > 0.0
        shares = []
        for h in range(local_heads):
            score = score_ref[j, h * every : (h + 1) * every, :]
            score = score * scale + bias_score[h : h + 1, :]
            score = jnp.where(live, score, -1e30)
            expo = jnp.exp(score - jnp.max(score, axis=0, keepdims=True))
            prob = expo * (1.0 / jnp.sum(expo, axis=0, keepdims=True))
            whole = jnp.broadcast_to(jnp.sum(prob, axis=0, keepdims=True), (8, half))
            shares.append(jnp.concatenate([prob * scale, whole], axis=0))
        wide = jnp.dot(
            widen, jnp.concatenate(shares, axis=1).astype(BF16), preferred_element_type=F32
        )
        for h in range(local_heads):
            weight = wide[:, h * half : (h + 1) * half] * field_ref[j]
            weight_ref[j, :, h * rows : (h + 1) * rows] = weight.T.astype(BF16)

    for get in get_values:
        get.wait()
    strip_heads = local_heads // halves
    of_column = lax.broadcasted_iota(jnp.int32, (rows, strip), 1) // head_size
    for a in range(halves):
        for src in rings:
            remote(
                value_all.at[a, src],
                value_all.at[a, src],
                send_sem.at[2],
                value_rs.at[a, src],
                here,
            ).wait_recv()
        projected = jnp.dot(
            left[...],
            value_all[a].reshape(hi_size * depth, strip),
            preferred_element_type=F32,
        )
        sent = 0
        for j in range(lo_size):
            part = projected[j * rows : (j + 1) * rows]
            spread = jnp.concatenate(
                [jnp.where(of_column == h, part, 0.0) for h in range(strip_heads)], axis=0
            ).astype(BF16)
            these = slice(a * strip_heads * rows, (a + 1) * strip_heads * rows)
            mixed = jnp.dot(weight_ref[j, :, these], spread, preferred_element_type=F32)
            mix_send[a, j * groups : (j + 1) * groups] = mixed.astype(BF16).reshape(
                groups, owned, strip
            )
            ready = (j + 1) * groups - 1
            for k in range(sent, ready):
                to = other_than(mixer, k)
                to_lo = lax.div(to, groups)
                there = {"dp": first_b + to_lo, "var": (r - to_lo) * groups + to}
                remote(
                    mix_send.at[a, to],
                    mix_recv.at[a, mixer],
                    send_sem.at[5],
                    mix_rs.at[a, mixer],
                    there,
                ).start()
            sent = ready

    get_out.wait()
    total = jnp.zeros((owned, width), F32)
    for a in range(halves):
        for near in range(groups):
            summed = None
            for far in range(lo_size):
                bits = far * groups + near
                src, _ = partner_of(bits)
                if bits:
                    remote(
                        mix_send.at[a, src],
                        mix_recv.at[a, src],
                        send_sem.at[5],
                        mix_rs.at[a, src],
                        here,
                    ).wait_recv()
                    part = mix_recv[a, src].astype(F32)
                else:
                    part = mix_send[a, src].astype(F32)
                summed = part if summed is None else summed + part
            total += jnp.dot(
                summed.astype(BF16),
                wout[strip_of(my_v.flip(near) - r * groups, a), :],
                preferred_element_type=F32,
            )
    result_ref[0] = total.astype(result_ref.dtype)

    all_ids.wait_send()
    all_pixels.wait_send()
    all_folds.wait_send()
    all_scales.wait_send()
    for a in range(halves):
        arrived(value_all.at[a], hi_size - 1, send_sem.at[2], value_rs.at[0, 0]).wait_send()
        arrived(mix_send.at[a], mixers - 1, send_sem.at[5], mix_rs.at[0, 0]).wait_send()


def on_device(
    n,
    nv,
    pixels,
    var_ids,
    counts,
    patch_weight,
    var_embed,
    norm_gain,
    norm_bias,
    key_weight,
    value_weight,
    query,
    out_weight,
):
    slots, taps, patches = pixels.shape[1:]
    width = out_weight.shape[0]
    heads, head_size = query.shape
    groups = min(nv, width // 128)
    lo_size = 2 if n % 2 == 0 else 1
    hi_size = n // lo_size
    team = lo_size * nv
    mixers = lo_size * groups
    columns = width // groups
    halves = 2 if columns % 256 == 0 else 1
    strip = columns // halves
    depth = value_weight.shape[0]
    padded = rounded_up(slots, 8)
    owned = patches // nv
    half = patches * groups // nv
    local_heads = heads // groups
    fold_rows = rounded_up(local_heads, 8)
    every = nv * slots
    rows = rounded_up(every * taps + every + 1, 16)
    hbm = pl.BlockSpec(memory_space=pltpu.HBM)
    vmem = pl.BlockSpec(memory_space=pltpu.VMEM)
    dims = (n, nv, groups, lo_size, slots, taps, patches, width, heads, head_size)
    dma = pltpu.SemaphoreType.DMA
    return pl.pallas_call(
        functools.partial(kernel, dims),
        out_shape=pltpu.VMEM((1, owned, width), BF16),
        in_specs=[hbm] * 11,
        out_specs=vmem,
        scratch_shapes=[
            pltpu.SMEM((team,) + var_ids.shape, jnp.int32),
            pltpu.SMEM(counts.shape, jnp.int32),
            pltpu.VMEM((team, slots, taps, patches), BF16),
            pltpu.VMEM(patch_weight.shape, BF16),
            pltpu.VMEM(var_embed.shape, BF16),
            pltpu.VMEM((1, width), F32),
            pltpu.VMEM((1, width), F32),
            pltpu.VMEM(query.shape, F32),
            pltpu.VMEM((depth, columns), BF16),
            pltpu.VMEM((halves, depth, strip), BF16),
            pltpu.VMEM((halves, hi_size, depth, strip), BF16),
            pltpu.VMEM((width, width), BF16),
            pltpu.VMEM((n, fold_rows, depth), F32),
            pltpu.VMEM((taps + 1, padded, width), F32),
            pltpu.VMEM((lo_size, rows, width), F32),
            pltpu.VMEM((lo_size * rows, hi_size * depth), BF16),
            pltpu.VMEM((lo_size, rows, half), F32),
            pltpu.VMEM((team, padded, patches), F32),
            pltpu.VMEM((lo_size, every, half), F32),
            pltpu.VMEM((lo_size, local_heads * every, half), F32),
            pltpu.VMEM((lo_size, half, local_heads * rows), BF16),
            pltpu.VMEM((halves, mixers, owned, strip), BF16),
            pltpu.VMEM((halves, mixers, owned, strip), BF16),
            dma((10 + 2 * halves,)),
            dma((6,)),
            dma((4,)),
            dma((halves, hi_size)),
            dma((halves, mixers)),
            pltpu.SemaphoreType.REGULAR,
        ],
        compiler_params=pltpu.CompilerParams(collective_id=0, has_side_effects=True),
    )(
        pixels,
        var_ids,
        counts,
        patch_weight,
        var_embed,
        norm_gain.reshape(1, width),
        norm_bias.reshape(1, width),
        key_weight,
        value_weight,
        query,
        out_weight,
    )


def solution(mesh):
    placed = (
        P("dp", "var", None, None),
        P("dp", "var"),
        P("dp"),
        P(),
        P(),
        P(),
        P(),
        P("dp", None),
        P("dp", None),
        P(),
        P(),
    )
    return jax.shard_map(
        functools.partial(on_device, mesh.shape["dp"], mesh.shape["var"]),
        mesh=mesh,
        in_specs=placed,
        out_specs=P("dp", "var", None),
        check_vma=False,
    )
```

```python
import functools
import math

import jax
import jax.numpy as jnp
from jax import lax
from jax.experimental import pallas as pl
from jax.experimental.pallas import tpu as pltpu
from jax.sharding import PartitionSpec as P

F32 = jnp.float32
BF16 = jnp.bfloat16
MESH = pl.DeviceIdType.MESH
PIECES = 3


def rounded_up(value, unit):
    return -(-value // unit) * unit


class Bits:
    def __init__(self, index, size):
        self.index = index
        self.steps = {}
        bit = 1
        while bit < size:
            self.steps[bit] = bit - 2 * bit * lax.rem(lax.div(index, bit), 2)
            bit *= 2

    def flip(self, bits):
        index = self.index
        for bit, step in self.steps.items():
            if bits & bit:
                index = index + step
        return index


def pieces_of(value):
    parts = []
    for _ in range(PIECES):
        part = value.astype(BF16).astype(F32)
        parts.append(part)
        value = value - part
    return parts


def kernel(
    dims,
    pixels_hbm,
    ids_hbm,
    counts_hbm,
    table_hbm,
    embed_hbm,
    gain_hbm,
    bias_hbm,
    key_hbm,
    value_hbm,
    query_hbm,
    out_hbm,
    result_ref,
    ids_all,
    counts_ref,
    pix_all,
    table,
    embed,
    gain_ref,
    bias_ref,
    query_ref,
    key_block,
    value_send,
    value_all,
    wout,
    fold_all,
    own_rows,
    raw,
    left,
    field_ref,
    scale_all,
    scale_ref,
    score_ref,
    weight_ref,
    mix_send,
    mix_recv,
    local_sem,
    send_sem,
    once_sem,
    value_rs,
    mix_rs,
    hand,
):
    n, nv, groups, lo_size, slots, taps, patches, width, heads, head_size = dims
    hi_size = n // lo_size
    team = lo_size * nv
    mixers = lo_size * groups
    depth = key_block.shape[0]
    columns = key_block.shape[1]
    halves = value_all.shape[0]
    strip = columns // halves
    crossed = groups % 2 == 0
    local_heads = heads // groups
    fold_rows = fold_all.shape[1]
    half = patches * groups // nv
    owned = patches // nv
    padded = own_rows.shape[1]
    every = nv * slots
    tap_rows = every * taps
    rows = raw.shape[1]
    tail = rows - tap_rows - every

    b = lax.axis_index("dp")
    v = lax.axis_index("var")
    hi, lo = lax.div(b, lo_size), lax.rem(b, lo_size)
    r, g = lax.div(v, groups), lax.rem(v, groups)
    me = lo * nv + v
    mixer = lo * groups + g
    my_lo, my_v = Bits(lo, lo_size), Bits(v, nv)
    first_b = b - lo

    def mate(bits):
        return {"dp": first_b + my_lo.flip(bits // nv), "var": my_v.flip(bits % nv)}

    def partner_of(bits):
        far, near = bits // groups, bits % groups
        there = my_v.flip(near)
        return my_lo.flip(far) * groups + there - r * groups, {
            "dp": first_b + my_lo.flip(far),
            "var": there,
        }

    def other_than(index, k):
        return k + jnp.where(index <= k, 1, 0)

    rings = [other_than(hi, k) for k in range(hi_size - 1)]

    def remote(src, dst, ss, rs, where):
        return pltpu.make_async_remote_copy(
            src_ref=src, dst_ref=dst, send_sem=ss, recv_sem=rs, device_id=where, device_id_type=MESH
        )

    here = {"dp": b, "var": v}
    to_core = my_v.flip(1) if crossed else v
    to_group = to_core - r * groups

    mine = pl.ds(pl.multiple_of(g * columns, columns), columns)

    def strip_of(group, a):
        return pl.ds(pl.multiple_of(group * columns + a * strip, strip), strip)

    copies = [
        (query_hbm, query_ref),
        (key_hbm.at[:, mine], key_block),
        (ids_hbm, ids_all.at[me]),
        (pixels_hbm.at[0], pix_all.at[me]),
        (table_hbm, table),
        (embed_hbm, embed),
        (gain_hbm, gain_ref),
        (bias_hbm, bias_ref),
        (counts_hbm, counts_ref),
        (out_hbm, wout),
    ]
    copies += [(value_hbm.at[:, strip_of(g, a)], value_all.at[a, hi]) for a in range(halves)]
    copies[2:2] = [
        (value_hbm.at[:, strip_of(to_group, a)], value_send.at[a]) for a in range(halves)
    ]
    gets = [pltpu.make_async_copy(s, d, local_sem.at[i]) for i, (s, d) in enumerate(copies)]
    for get in gets:
        get.start()

    barrier = pltpu.get_barrier_semaphore()

    def greet(where):
        pl.semaphore_signal(barrier, inc=1, device_id=where, device_id_type=MESH)

    core = lax.rem(v, 2)
    partner = {"var": my_v.flip(1)}
    if crossed:
        for k, to in enumerate(rings):
            ear = 1 if k == 0 else jnp.where(hi == 0, 1, 0)
            for other in range(lo_size):
                greet({"dp": to * lo_size + other, "var": v - core + ear})

        @pl.when(core == 0)
        def _():
            greet(partner)
            for bits in range(2, team, 2):
                greet(mate(bits))

        @pl.when(core == 1)
        def _():
            for bits in range(1, team, 2):
                greet(mate(bits))
    else:
        for to in rings:
            for other in range(lo_size):
                greet({"dp": to * lo_size + other})
        for bits in range(1, team):
            greet(mate(bits))

    get_query, get_key = gets[:2]
    get_strips = gets[2 : 2 + halves]
    get_values = gets[-halves:]
    (
        get_ids,
        get_pixels,
        get_table,
        get_embed,
        get_gain,
        get_bias,
        get_counts,
        get_out,
    ) = gets[2 + halves : -halves]

    get_query.wait()
    own_query = query_ref[:local_heads]
    for i in range(1, groups):
        own_query = jnp.where(
            g == i, query_ref[i * local_heads : (i + 1) * local_heads], own_query
        )
    own_query = own_query * (1.0 / math.sqrt(head_size))
    if fold_rows > local_heads:
        blank = jnp.zeros((fold_rows - local_heads, head_size), F32)
        own_query = jnp.concatenate([own_query, blank], axis=0)
    own_head = (
        lax.broadcasted_iota(jnp.int32, (fold_rows, columns), 1) // head_size
        == lax.broadcasted_iota(jnp.int32, (fold_rows, columns), 0)
    )
    diagonal = jnp.where(own_head, jnp.concatenate([own_query] * local_heads, axis=1), 0.0)
    diagonal = jnp.concatenate(pieces_of(diagonal), axis=0).astype(BF16)
    get_key.wait()
    found = lax.dot_general(
        diagonal, key_block[...], (((1,), (1,)), ((), ())), preferred_element_type=F32
    )
    fold = found[:fold_rows]
    for i in range(1, PIECES):
        fold = fold + found[i * fold_rows : (i + 1) * fold_rows]
    fold_all[b] = fold

    for get in get_strips:
        get.wait()
    get_ids.wait()
    get_pixels.wait()

    def send_fold(there):
        remote(fold_all.at[b], fold_all.at[b], send_sem.at[3], once_sem.at[2], there).start()

    def send_folds(some):
        for to in some:
            for other in range(lo_size):
                send_fold({"dp": to * lo_size + other})

    def send_values(some, strips):
        for a in strips:
            for to in some:
                there = {"dp": to * lo_size + lo, "var": to_core}
                remote(
                    value_send.at[a],
                    value_all.at[a, hi],
                    send_sem.at[2],
                    value_rs.at[a, hi],
                    there,
                ).start()

    def send_rows(some):
        send_folds(some)
        send_values(some, range(halves))

    def send_first():
        send_folds(rings[:1])
        send_values(rings[:1], range(1))

    def send_rest():
        send_folds(rings[1:])
        send_values(rings[:1], range(1, halves))
        send_values(rings[1:], range(halves))

    def send_team():
        for bits in range(1, team):
            where = mate(bits)
            remote(ids_all.at[me], ids_all.at[me], send_sem.at[0], once_sem.at[0], where).start()
            remote(pix_all.at[me], pix_all.at[me], send_sem.at[1], once_sem.at[1], where).start()
        for far in range(1, lo_size):
            send_fold({"dp": first_b + my_lo.flip(far)})

    def tell_partner():
        pl.semaphore_signal(hand, inc=1, device_id=partner, device_id_type=MESH)

    if crossed:
        early, even = hi == 0, core == 0

        @pl.when(early & even)
        def _():
            pl.semaphore_wait(barrier, team - 1)
            tell_partner()
            send_team()
            pl.semaphore_wait(hand, 1)
            send_rows(rings)

        @pl.when(early & ~even)
        def _():
            pl.semaphore_wait(hand, 1)
            send_team()
            pl.semaphore_wait(barrier, 2 * (n - lo_size) + 1)
            tell_partner()
            send_rows(rings)

        @pl.when(~early & even)
        def _():
            pl.semaphore_wait(hand, 1)
            send_first()
            pl.semaphore_wait(barrier, team - 1 + 2 * (n - 2 * lo_size))
            tell_partner()
            send_rest()
            send_team()

        @pl.when(~early & ~even)
        def _():
            pl.semaphore_wait(barrier, 2 * lo_size + 1)
            tell_partner()
            send_first()
            pl.semaphore_wait(hand, 1)
            send_rest()
            send_team()

    else:
        pl.semaphore_wait(barrier, n - lo_size + team - 1)
        send_rows(rings)
        send_team()

    get_table.wait()
    get_embed.wait()
    own_rows[...] = jnp.zeros_like(own_rows)
    ids_at = lax.broadcasted_iota(jnp.int32, (padded, embed.shape[0]), 0)
    wanted = jnp.full((padded, embed.shape[0]), -1, jnp.int32)
    for s in range(slots):
        chosen = ids_all[me, 0, s]
        found = table[chosen].astype(F32)
        for k in range(taps):
            own_rows[k, s : s + 1, :] = found[k : k + 1, :]
        wanted = jnp.where(ids_at == s, chosen, wanted)
    hot = (wanted == lax.broadcasted_iota(jnp.int32, wanted.shape, 1)).astype(BF16)
    own_rows[taps] = jnp.dot(hot, embed[...], preferred_element_type=F32)
    centred = []
    for k in range(taps + 1):
        row = own_rows[k]
        centred.append(row - jnp.mean(row, axis=-1, keepdims=True))
    pix = pix_all[me].astype(F32)
    fill = jnp.zeros((padded - slots, patches), F32)
    field = []
    for k in range(taps):
        own = [pix[s, k : k + 1, :] for s in range(slots)]
        field.append(jnp.concatenate(own + ([fill] if padded > slots else []), axis=0))
    field.append(jnp.ones((padded, patches), F32))
    variance = jnp.zeros((padded, patches), F32)
    for k in range(taps + 1):
        for m in range(k, taps + 1):
            gram = jnp.mean(centred[k] * centred[m], axis=-1, keepdims=True)
            variance += (1.0 if m == k else 2.0) * gram * (field[k] * field[m])
    scale = lax.rsqrt(jnp.maximum(variance, 0.0) + 1e-05)
    get_counts.wait()
    place = lax.broadcasted_iota(jnp.int32, (padded, patches), 0)
    live = (place < slots) & (v * slots + place < counts_ref[0])
    scale_all[me] = jnp.where(live, scale, -1.0)
    for bits in range(team - 1, 0, -1):
        remote(
            scale_all.at[me], scale_all.at[me], send_sem.at[4], once_sem.at[3], mate(bits)
        ).start()

    def arrived(ref, count, ss, rs):
        block = ref.at[pl.ds(0, count)]
        return remote(block, block, ss, rs, here)

    all_ids = arrived(ids_all, team - 1, send_sem.at[0], once_sem.at[0])
    all_ids.wait_recv()
    get_gain.wait()
    get_bias.wait()
    gain = gain_ref[...]
    slot_at = lax.broadcasted_iota(jnp.int32, (every, embed.shape[0]), 0)
    for j in range(lo_size):
        wanted = jnp.full((every, embed.shape[0]), -1, jnp.int32)
        for s in range(every):
            chosen = ids_all[j * nv + s // slots, 0, s % slots]
            raw[j, s * taps : (s + 1) * taps, :] = table[chosen].astype(F32)
            wanted = jnp.where(slot_at == s, chosen, wanted)
        hot = (wanted == lax.broadcasted_iota(jnp.int32, wanted.shape, 1)).astype(BF16)
        raw[j, tap_rows : tap_rows + every, :] = jnp.dot(
            hot, embed[...], preferred_element_type=F32
        )
        raw[j, tap_rows + every :, :] = jnp.zeros((tail, width), F32)
        row = raw[j, : tap_rows + every, :]
        row = (row - jnp.mean(row, axis=-1, keepdims=True)) * gain
        last = lax.broadcasted_iota(jnp.int32, (tail, width), 0)
        last = jnp.where(last == 0, bias_ref[...], 0.0)
        basis = jnp.concatenate([row, last], axis=0)
        parts = []
        for h in range(hi_size):
            at = h * lo_size * depth
            part = basis[:, at : at + depth]
            for other in range(1, lo_size):
                at += depth
                part = jnp.where(lo == other, basis[:, at : at + depth], part)
            parts.append(part)
        left[j * rows : (j + 1) * rows, :] = jnp.concatenate(parts, axis=1).astype(BF16)

    all_pixels = arrived(pix_all, team - 1, send_sem.at[1], once_sem.at[1])
    all_pixels.wait_recv()
    window = pl.ds(pl.multiple_of(r * half, half), half)
    for j in range(lo_size):
        for s in range(every):
            field_ref[j, s * taps : (s + 1) * taps, :] = pix_all[
                j * nv + s // slots, s % slots, :, window
            ].astype(F32)
        field_ref[j, tap_rows:, :] = jnp.ones((rows - tap_rows, half), F32)

    all_folds = arrived(fold_all, n - 1, send_sem.at[3], once_sem.at[2])
    all_folds.wait_recv()
    folded = jnp.concatenate([fold_all[i] for i in range(n)], axis=1)
    bias_score = jnp.sum(folded * bias_ref[...], axis=-1, keepdims=True)
    folded = folded * gain
    fold_sum = jnp.sum(folded, axis=-1, keepdims=True)
    keys = jnp.concatenate(pieces_of(folded) + [jnp.ones((8, width), F32)], axis=0).astype(BF16)

    which = lax.broadcasted_iota(jnp.int32, (every, rows), 0)
    what = lax.broadcasted_iota(jnp.int32, (every, rows), 1)
    of_slot = jnp.where(what < tap_rows, what // taps, what - tap_rows) == which
    to_row = lax.broadcasted_iota(jnp.int32, (rows, every + 8), 0)
    of_row = jnp.where(to_row < tap_rows, to_row // taps, to_row - tap_rows)
    widen = (of_row == lax.broadcasted_iota(jnp.int32, (rows, every + 8), 1)).astype(BF16)

    blocks = []
    for j in range(lo_size):
        found = lax.dot_general(
            keys, raw[j].astype(BF16), (((1,), (1,)), ((), ())), preferred_element_type=F32
        )
        score_of = found[:fold_rows]
        for i in range(1, PIECES):
            score_of = score_of + found[i * fold_rows : (i + 1) * fold_rows]
        row_sum = found[PIECES * fold_rows : PIECES * fold_rows + 1]
        score_of = score_of - (row_sum * (1.0 / width)) * fold_sum
        parts = [
            jnp.where(of_slot, part[h : h + 1, :], 0.0)
            for part in pieces_of(score_of)
            for h in range(local_heads)
        ]
        blocks.append(jnp.concatenate(parts, axis=0).astype(BF16))

    for j in range(lo_size):
        found = jnp.dot(blocks[j], field_ref[j].astype(BF16), preferred_element_type=F32)
        every_head = local_heads * every
        score = found[:every_head]
        for i in range(1, PIECES):
            score = score + found[i * every_head : (i + 1) * every_head]
        score_ref[j] = score

    all_scales = arrived(scale_all, team - 1, send_sem.at[4], once_sem.at[3])
    all_scales.wait_recv()
    for j in range(lo_size):
        for i in range(nv):
            scale_ref[j, i * slots : (i + 1) * slots, :] = scale_all[j * nv + i, :slots, window]
        scale = scale_ref[j]
        live = scale > 0.0
        shares = []
        for h in range(local_heads):
            score = score_ref[j, h * every : (h + 1) * every, :]
            score = score * scale + bias_score[h : h + 1, :]
            score = jnp.where(live, score, -1e30)
            expo = jnp.exp(score - jnp.max(score, axis=0, keepdims=True))
            prob = expo * (1.0 / jnp.sum(expo, axis=0, keepdims=True))
            whole = jnp.broadcast_to(jnp.sum(prob, axis=0, keepdims=True), (8, half))
            shares.append(jnp.concatenate([prob * scale, whole], axis=0))
        wide = jnp.dot(
            widen, jnp.concatenate(shares, axis=1).astype(BF16), preferred_element_type=F32
        )
        for h in range(local_heads):
            weight = wide[:, h * half : (h + 1) * half] * field_ref[j]
            weight_ref[j, :, h * rows : (h + 1) * rows] = weight.T.astype(BF16)

    for get in get_values:
        get.wait()
    strip_heads = local_heads // halves
    of_column = lax.broadcasted_iota(jnp.int32, (rows, strip), 1) // head_size
    for a in range(halves):
        for src in rings:
            remote(
                value_all.at[a, src],
                value_all.at[a, src],
                send_sem.at[2],
                value_rs.at[a, src],
                here,
            ).wait_recv()
        projected = jnp.dot(
            left[...],
            value_all[a].reshape(hi_size * depth, strip),
            preferred_element_type=F32,
        )
        sent = 0
        for j in range(lo_size):
            part = projected[j * rows : (j + 1) * rows]
            spread = jnp.concatenate(
                [jnp.where(of_column == h, part, 0.0) for h in range(strip_heads)], axis=0
            ).astype(BF16)
            these = slice(a * strip_heads * rows, (a + 1) * strip_heads * rows)
            mixed = jnp.dot(weight_ref[j, :, these], spread, preferred_element_type=F32)
            mix_send[a, j * groups : (j + 1) * groups] = mixed.astype(BF16).reshape(
                groups, owned, strip
            )
            ready = (j + 1) * groups - 1
            for k in range(sent, ready):
                to = other_than(mixer, k)
                to_lo = lax.div(to, groups)
                there = {"dp": first_b + to_lo, "var": (r - to_lo) * groups + to}
                remote(
                    mix_send.at[a, to],
                    mix_recv.at[a, mixer],
                    send_sem.at[5],
                    mix_rs.at[a, mixer],
                    there,
                ).start()
            sent = ready

    get_out.wait()
    total = jnp.zeros((owned, width), F32)
    for a in range(halves):
        for near in range(groups):
            summed = None
            for far in range(lo_size):
                bits = far * groups + near
                src, _ = partner_of(bits)
                if bits:
                    remote(
                        mix_send.at[a, src],
                        mix_recv.at[a, src],
                        send_sem.at[5],
                        mix_rs.at[a, src],
                        here,
                    ).wait_recv()
                    part = mix_recv[a, src].astype(F32)
                else:
                    part = mix_send[a, src].astype(F32)
                summed = part if summed is None else summed + part
            total += jnp.dot(
                summed.astype(BF16),
                wout[strip_of(my_v.flip(near) - r * groups, a), :],
                preferred_element_type=F32,
            )
    result_ref[0] = total.astype(result_ref.dtype)

    all_ids.wait_send()
    all_pixels.wait_send()
    all_folds.wait_send()
    all_scales.wait_send()
    for a in range(halves):
        arrived(value_all.at[a], hi_size - 1, send_sem.at[2], value_rs.at[0, 0]).wait_send()
        arrived(mix_send.at[a], mixers - 1, send_sem.at[5], mix_rs.at[0, 0]).wait_send()


def on_device(
    n,
    nv,
    pixels,
    var_ids,
    counts,
    patch_weight,
    var_embed,
    norm_gain,
    norm_bias,
    key_weight,
    value_weight,
    query,
    out_weight,
):
    slots, taps, patches = pixels.shape[1:]
    width = out_weight.shape[0]
    heads, head_size = query.shape
    groups = min(nv, width // 128)
    lo_size = 2 if n % 2 == 0 else 1
    hi_size = n // lo_size
    team = lo_size * nv
    mixers = lo_size * groups
    columns = width // groups
    halves = 2 if columns % 256 == 0 else 1
    strip = columns // halves
    depth = value_weight.shape[0]
    padded = rounded_up(slots, 8)
    owned = patches // nv
    half = patches * groups // nv
    local_heads = heads // groups
    fold_rows = rounded_up(local_heads, 8)
    every = nv * slots
    rows = rounded_up(every * taps + every + 1, 16)
    hbm = pl.BlockSpec(memory_space=pltpu.HBM)
    vmem = pl.BlockSpec(memory_space=pltpu.VMEM)
    dims = (n, nv, groups, lo_size, slots, taps, patches, width, heads, head_size)
    dma = pltpu.SemaphoreType.DMA
    return pl.pallas_call(
        functools.partial(kernel, dims),
        out_shape=pltpu.VMEM((1, owned, width), BF16),
        in_specs=[hbm] * 11,
        out_specs=vmem,
        scratch_shapes=[
            pltpu.SMEM((team,) + var_ids.shape, jnp.int32),
            pltpu.SMEM(counts.shape, jnp.int32),
            pltpu.VMEM((team, slots, taps, patches), BF16),
            pltpu.VMEM(patch_weight.shape, BF16),
            pltpu.VMEM(var_embed.shape, BF16),
            pltpu.VMEM((1, width), F32),
            pltpu.VMEM((1, width), F32),
            pltpu.VMEM(query.shape, F32),
            pltpu.VMEM((depth, columns), BF16),
            pltpu.VMEM((halves, depth, strip), BF16),
            pltpu.VMEM((halves, hi_size, depth, strip), BF16),
            pltpu.VMEM((width, width), BF16),
            pltpu.VMEM((n, fold_rows, depth), F32),
            pltpu.VMEM((taps + 1, padded, width), F32),
            pltpu.VMEM((lo_size, rows, width), F32),
            pltpu.VMEM((lo_size * rows, hi_size * depth), BF16),
            pltpu.VMEM((lo_size, rows, half), F32),
            pltpu.VMEM((team, padded, patches), F32),
            pltpu.VMEM((lo_size, every, half), F32),
            pltpu.VMEM((lo_size, local_heads * every, half), F32),
            pltpu.VMEM((lo_size, half, local_heads * rows), BF16),
            pltpu.VMEM((halves, mixers, owned, strip), BF16),
            pltpu.VMEM((halves, mixers, owned, strip), BF16),
            dma((10 + 2 * halves,)),
            dma((6,)),
            dma((4,)),
            dma((halves, hi_size)),
            dma((halves, mixers)),
            pltpu.SemaphoreType.REGULAR,
        ],
        compiler_params=pltpu.CompilerParams(collective_id=0, has_side_effects=True),
    )(
        pixels,
        var_ids,
        counts,
        patch_weight,
        var_embed,
        norm_gain.reshape(1, width),
        norm_bias.reshape(1, width),
        key_weight,
        value_weight,
        query,
        out_weight,
    )


def solution(mesh):
    placed = (
        P("dp", "var", None, None),
        P("dp", "var"),
        P("dp"),
        P(),
        P(),
        P(),
        P(),
        P("dp", None),
        P("dp", None),
        P(),
        P(),
    )
    return jax.shard_map(
        functools.partial(on_device, mesh.shape["dp"], mesh.shape["var"]),
        mesh=mesh,
        in_specs=placed,
        out_specs=P("dp", "var", None),
        check_vma=False,
    )
```
